8 devices in a mesh: sp: 8 (over z, y, x, core).
Axes of the slice: x: 2, y: 2, z: 1, core: 2. Of those that a mesh axis runs over, the one named last changes fastest.
Arguments:
- hidden: bfloat16 [32, 512, 1024], P(None, 'sp')
- norm_gain: float32 [1024], replicated
- w_q: bfloat16 [1024, 2048], replicated
- w_k: bfloat16 [1024, 1024], replicated
- w_v: bfloat16 [1024, 1024], replicated
- q_gain: float32 [128], replicated
- k_gain: float32 [128], replicated
- w_o: bfloat16 [2048, 1024], replicated
- d_out: bfloat16 [32, 512, 1024], P(None, 'sp')
Outputs:
- output 1: bfloat16 [32, 512, 1024], P(None, 'sp')
- output 2: bfloat16 [32, 512, 1024], P(None, 'sp')
- output 3: float32 [1024, 2048], replicated
- output 4: float32 [1024, 1024], replicated
- output 5: float32 [1024, 1024], replicated
- output 6: float32 [2048, 1024], replicated
- output 7: float32 [1024], replicated
- output 8: float32 [128], replicated
- output 9: float32 [128], replicated
All inputs are finite; a program needn't handle non-finite values.
Results may differ from the reference program's by a relative error of at most 0.0177018.
Values are sent between devices in bfloat16 or wider.
A program may use at most 1 GiB of HBM per device.

```python
import math
import jax
import jax.numpy as jnp
from jax import lax

BATCH_SIZE = 32
SEQ_LEN = 512
MODEL_DIM = 1024
Q_HEADS = 16
KV_HEADS = 8
HEAD_DIM = 128
ROPE_BASE = 1000000
NORM_EPS = 1e-6


def setup_inputs(seed: int = 0) -> dict:
    keys = jax.random.split(jax.random.key(seed), 9)
    q_width = Q_HEADS * HEAD_DIM
    kv_width = KV_HEADS * HEAD_DIM
    hidden = jax.random.normal(keys[0], (BATCH_SIZE, SEQ_LEN, MODEL_DIM), jnp.float32)
    norm_gain = 1.0 + 0.5 * jax.random.normal(keys[1], (MODEL_DIM,), jnp.float32)
    w_q = jax.random.normal(keys[2], (MODEL_DIM, q_width), jnp.float32) * MODEL_DIM ** -0.5
    w_k = jax.random.normal(keys[3], (MODEL_DIM, kv_width), jnp.float32) * MODEL_DIM ** -0.5
    w_v = jax.random.normal(keys[4], (MODEL_DIM, kv_width), jnp.float32) * MODEL_DIM ** -0.5
    q_gain = 1.0 + 0.3 * jax.random.normal(keys[5], (HEAD_DIM,), jnp.float32)
    k_gain = 1.0 + 0.3 * jax.random.normal(keys[6], (HEAD_DIM,), jnp.float32)
    w_o = jax.random.normal(keys[7], (q_width, MODEL_DIM), jnp.float32) * q_width ** -0.5
    d_out = jax.random.normal(keys[8], (BATCH_SIZE, SEQ_LEN, MODEL_DIM), jnp.float32)
    return {'hidden': hidden.astype(jnp.bfloat16), 'norm_gain': norm_gain, 'w_q': w_q.astype(jnp.bfloat16), 'w_k': w_k.astype(jnp.bfloat16), 'w_v': w_v.astype(jnp.bfloat16), 'q_gain': q_gain, 'k_gain': k_gain, 'w_o': w_o.astype(jnp.bfloat16), 'd_out': d_out.astype(jnp.bfloat16)}


def rms_scale(values, gain):
    return values * lax.rsqrt(jnp.mean(values * values, axis=-1, keepdims=True) + NORM_EPS) * gain


def rope_tables(positions):
    half_dim = HEAD_DIM // 2
    inv_freq = jnp.exp(jnp.arange(half_dim).astype(jnp.float32) * (-2.0 * math.log(ROPE_BASE) / HEAD_DIM))
    angles = positions[:, None] * inv_freq[None, :]
    return jnp.cos(angles), jnp.sin(angles)


def qk_post(raw, gain, cos_tab, sin_tab):
    normed = rms_scale(raw, gain)
    half_dim = HEAD_DIM // 2
    first = normed[..., :half_dim]
    second = normed[..., half_dim:]
    cos_b = cos_tab[None, :, None, :]
    sin_b = sin_tab[None, :, None, :]
    return jnp.concatenate([first * cos_b - second * sin_b, second * cos_b + first * sin_b], axis=-1)


def head_attn(q_head, k_head, v_head):
    n_pos = q_head.shape[1]
    scores = jnp.einsum('bqd,bkd->bqk', q_head, k_head) * HEAD_DIM ** -0.5
    causal = jnp.arange(n_pos)[:, None] >= jnp.arange(n_pos)[None, :]
    scores = jnp.where(causal[None], scores, -1e30)
    attn_prob = jax.nn.softmax(scores, axis=-1)
    attn_prob = attn_prob + lax.stop_gradient(attn_prob.astype(jnp.bfloat16).astype(jnp.float32) - attn_prob)
    return jnp.einsum('bqk,bkd->bqd', attn_prob, v_head)


def reference(hidden, norm_gain, w_q, w_k, w_v, q_gain, k_gain, w_o, d_out):
    group_size = Q_HEADS // KV_HEADS
    tokens = BATCH_SIZE * SEQ_LEN
    hidden_f = hidden.astype(jnp.float32)
    normed_f, norm_back = jax.vjp(rms_scale, hidden_f, norm_gain)
    flat_norm = normed_f.astype(jnp.bfloat16).reshape(tokens, MODEL_DIM)
    q_raw = jnp.dot(flat_norm, w_q, preferred_element_type=jnp.float32).astype(jnp.bfloat16)
    k_raw = jnp.dot(flat_norm, w_k, preferred_element_type=jnp.float32).astype(jnp.bfloat16)
    v_raw = jnp.dot(flat_norm, w_v, preferred_element_type=jnp.float32).astype(jnp.bfloat16)
    cos_tab, sin_tab = rope_tables(jnp.arange(SEQ_LEN).astype(jnp.float32))

    def post_both(q_in, k_in, q_scale, k_scale):
        return qk_post(q_in, q_scale, cos_tab, sin_tab), qk_post(k_in, k_scale, cos_tab, sin_tab)

    (q_rot, k_rot), post_back = jax.vjp(post_both, q_raw.astype(jnp.float32).reshape(BATCH_SIZE, SEQ_LEN, Q_HEADS, HEAD_DIM), k_raw.astype(jnp.float32).reshape(BATCH_SIZE, SEQ_LEN, KV_HEADS, HEAD_DIM), q_gain, k_gain)
    q_heads = jnp.moveaxis(q_rot.astype(jnp.bfloat16), 2, 0)
    k_heads = jnp.moveaxis(k_rot.astype(jnp.bfloat16), 2, 0)
    v_heads = jnp.moveaxis(v_raw.reshape(BATCH_SIZE, SEQ_LEN, KV_HEADS, HEAD_DIM), 2, 0)
    head_ids = jnp.arange(Q_HEADS)

    def fwd_one(head_item):
        q_head, head_id = head_item
        kv_id = head_id // group_size
        return head_attn(q_head.astype(jnp.float32), k_heads[kv_id].astype(jnp.float32), v_heads[kv_id].astype(jnp.float32))

    out_heads = lax.map(fwd_one, (q_heads, head_ids))
    attn = jnp.moveaxis(out_heads, 0, 2).astype(jnp.bfloat16).reshape(tokens, Q_HEADS * HEAD_DIM)
    y_out = (hidden_f.reshape(tokens, MODEL_DIM) + jnp.dot(attn, w_o, preferred_element_type=jnp.float32)).astype(jnp.bfloat16).reshape(BATCH_SIZE, SEQ_LEN, MODEL_DIM)
    dy_flat = d_out.reshape(tokens, MODEL_DIM)
    d_attn = jnp.dot(dy_flat, w_o.T, preferred_element_type=jnp.float32).astype(jnp.bfloat16)
    d_wo = jnp.dot(attn.T, dy_flat, preferred_element_type=jnp.float32)
    d_attn_heads = jnp.moveaxis(d_attn.reshape(BATCH_SIZE, SEQ_LEN, Q_HEADS, HEAD_DIM), 2, 0)

    def bwd_one(head_item):
        q_head, d_head, head_id = head_item
        kv_id = head_id // group_size
        _, head_back = jax.vjp(head_attn, q_head.astype(jnp.float32), k_heads[kv_id].astype(jnp.float32), v_heads[kv_id].astype(jnp.float32))
        return head_back(d_head.astype(jnp.float32))

    dq_heads, dk_each, dv_each = lax.map(bwd_one, (q_heads, d_attn_heads, head_ids))
    dk_heads = jnp.sum(dk_each.reshape(KV_HEADS, group_size, BATCH_SIZE, SEQ_LEN, HEAD_DIM), axis=1)
    dv_heads = jnp.sum(dv_each.reshape(KV_HEADS, group_size, BATCH_SIZE, SEQ_LEN, HEAD_DIM), axis=1)
    dq_all = jnp.moveaxis(dq_heads, 0, 2).astype(jnp.bfloat16)
    dk_all = jnp.moveaxis(dk_heads, 0, 2).astype(jnp.bfloat16)
    dv_flat = jnp.moveaxis(dv_heads, 0, 2).astype(jnp.bfloat16).reshape(tokens, KV_HEADS * HEAD_DIM)
    dq_raw_f, dk_raw_f, d_qgain, d_kgain = post_back((dq_all.astype(jnp.float32), dk_all.astype(jnp.float32)))
    dq_raw = dq_raw_f.astype(jnp.bfloat16).reshape(tokens, Q_HEADS * HEAD_DIM)
    dk_raw = dk_raw_f.astype(jnp.bfloat16).reshape(tokens, KV_HEADS * HEAD_DIM)
    d_wq = jnp.dot(flat_norm.T, dq_raw, preferred_element_type=jnp.float32)
    d_wk = jnp.dot(flat_norm.T, dk_raw, preferred_element_type=jnp.float32)
    d_wv = jnp.dot(flat_norm.T, dv_flat, preferred_element_type=jnp.float32)
    d_normed = jnp.dot(dq_raw, w_q.T, preferred_element_type=jnp.float32) + jnp.dot(dk_raw, w_k.T, preferred_element_type=jnp.float32) + jnp.dot(dv_flat, w_v.T, preferred_element_type=jnp.float32)
    dx_f, d_ngain = norm_back(d_normed.reshape(BATCH_SIZE, SEQ_LEN, MODEL_DIM))
    d_hidden = (d_out.astype(jnp.float32) + dx_f).astype(jnp.bfloat16)
    return (y_out, d_hidden, d_wq, d_wk, d_wv, d_wo, d_ngain, d_qgain, d_kgain)
```

```python
import math
import functools
import jax
import jax.numpy as jnp
from jax import lax
from jax.experimental import pallas as pl
from jax.experimental.pallas import tpu as pltpu
from jax.sharding import PartitionSpec as P

ROPE_BASE = 1000000.0
NORM_EPS = 1e-6
F32 = jnp.float32
BF16 = jnp.bfloat16
HD = 128
VMEM_LIMIT = 60 * 1024 * 1024


def rope_tables(n_pos):
    half = HD // 2
    inv_freq = jnp.exp(jnp.arange(half).astype(F32) * (-2.0 * math.log(ROPE_BASE) / HD))
    angles = jnp.arange(n_pos).astype(F32)[:, None] * inv_freq[None, :]
    cos, sin = jnp.cos(angles), jnp.sin(angles)
    return jnp.concatenate([cos, cos], axis=-1), jnp.concatenate([-sin, sin], axis=-1)


def qkv_kernel(x_ref, g_ref, wq_ref, wk_ref, wv_ref, gq_ref, gk_ref, cos_ref, sin_ref, h_ref, raw_ref, rot_ref):
    n_src, rows, tok, dim = x_ref.shape
    n = n_src * rows * tok
    x = x_ref[...].reshape(n, dim).astype(F32)
    r = lax.rsqrt(jnp.mean(x * x, axis=-1, keepdims=True) + NORM_EPS)
    h_ref[...] = (x * r * g_ref[...]).astype(BF16).reshape(h_ref.shape)
    cos = cos_ref[...].reshape(n_src, 1, tok, HD)
    sin = sin_ref[...].reshape(n_src, 1, tok, HD)

    def post(raw, gain):
        v = raw.astype(F32)
        v = v * lax.rsqrt(jnp.mean(v * v, axis=-1, keepdims=True) + NORM_EPS) * gain
        rolled = pltpu.roll(v, HD // 2, 1).reshape(n_src, rows, tok, HD)
        return (v.reshape(n_src, rows, tok, HD) * cos + rolled * sin).astype(BF16)

    gq, gk = gq_ref[...], gk_ref[...]
    shape = (n_src, rows, tok, HD)

    def body(j, _):
        hh = h_ref[...].reshape(n, dim)

        def proj(w_ref, width):
            cols = pl.ds(pl.multiple_of(j * width, width), width)
            return jnp.dot(hh, w_ref[:, cols], preferred_element_type=F32).astype(BF16)

        q, k, v = proj(wq_ref, 4 * HD), proj(wk_ref, 2 * HD), proj(wv_ref, 2 * HD)
        for i in range(2):
            heads = [q[:, 2 * i * HD:(2 * i + 1) * HD], q[:, (2 * i + 1) * HD:(2 * i + 2) * HD], k[:, i * HD:(i + 1) * HD]]
            for part, (val, gain) in enumerate(zip(heads, (gq, gq, gk))):
                raw_ref[:, :, :, pl.ds(pl.multiple_of((2 * j + i) * 3 * HD + part * HD, HD), HD)] = val.reshape(shape)
                rot_ref[:, :, :, pl.ds(pl.multiple_of((2 * j + i) * 4 * HD + part * HD, HD), HD)] = post(val, gain)
            rot_ref[:, :, :, pl.ds(pl.multiple_of((2 * j + i) * 4 * HD + 3 * HD, HD), HD)] = v[:, i * HD:(i + 1) * HD].reshape(shape)
        return 0

    lax.fori_loop(0, wk_ref.shape[1] // (2 * HD), body, 0, unroll=2)


QB = 256
NT = (((1,), (1,)), ((), ()))
EXP_SCALE = HD ** -0.5 * math.log2(math.e)


def softmax_t(k, q, qb):
    lo = qb * QB
    parts = [(lo, lax.dot_general(k[lo:lo + QB], q, NT, preferred_element_type=F32))]
    keys = lax.broadcasted_iota(jnp.int32, (QB, QB), 0)
    queries = lax.broadcasted_iota(jnp.int32, (QB, QB), 1)
    parts[0] = (lo, jnp.where(keys <= queries, parts[0][1], -1e30))
    if lo:
        parts.append((0, lax.dot_general(k[:lo], q, NT, preferred_element_type=F32)))
    top = functools.reduce(jnp.maximum, [jnp.max(s, axis=0, keepdims=True) for _, s in parts])
    exps = [(at, jnp.exp2((s - top) * EXP_SCALE)) for at, s in parts]
    inv = 1.0 / functools.reduce(jnp.add, [jnp.sum(e, axis=0, keepdims=True) for _, e in exps])
    return [(at, e * inv) for at, e in exps]


def attn_fwd_kernel(rot_ref, o_ref):
    n_pos = rot_ref.shape[0] * rot_ref.shape[2]
    rot = rot_ref[...].reshape(n_pos, 4 * HD)
    k, v_t = rot[:, 2 * HD:3 * HD], rot[:, 3 * HD:].T
    src_b = QB // rot_ref.shape[2]
    for qb in range(n_pos // QB):
        for head in range(2):
            q = rot[qb * QB:(qb + 1) * QB, head * HD:(head + 1) * HD]
            o_t = functools.reduce(jnp.add, [
                jnp.dot(v_t[:, at:at + p.shape[0]], p.astype(BF16), preferred_element_type=F32)
                for at, p in softmax_t(k, q, qb)])
            o_ref[pl.ds(qb * src_b, src_b), 0, :, pl.ds(head * HD, HD)] = o_t.T.astype(BF16).reshape(src_b, o_ref.shape[2], HD)


def attn_bwd_kernel(rot_ref, raw_ref, do_ref, gq_ref, gk_ref, cos_ref, sin_ref, oq_ref, ok_ref, ov_ref, dgq_ref, dgk_ref, dk_acc, dv_acc):
    n_src, _, tok, _ = rot_ref.shape
    n_pos = n_src * tok
    rot = rot_ref[...].reshape(n_pos, 4 * HD)
    raw = raw_ref[...].reshape(n_pos, 3 * HD)
    d_o = do_ref[...].reshape(n_pos, 2 * HD)
    k, v = rot[:, 2 * HD:3 * HD], rot[:, 3 * HD:]
    k_t = k.astype(F32).T.astype(BF16)
    src_b = QB // tok
    first = jnp.logical_and(pl.program_id(0) == 0, pl.program_id(1) == 0)

    @pl.when(first)
    def _():
        dgq_ref[...] = jnp.zeros_like(dgq_ref)
        dgk_ref[...] = jnp.zeros_like(dgk_ref)

    def post_back(d, x_raw, gain, lo, dg_ref):
        cnt = d.shape[0]
        d = d.astype(BF16).astype(F32)
        c, s = cos_ref[pl.ds(lo, cnt), :], sin_ref[pl.ds(lo, cnt), :]
        dn = d * c + pltpu.roll(d * s, HD // 2, 1)
        x = x_raw.astype(F32)
        r = lax.rsqrt(jnp.mean(x * x, axis=-1, keepdims=True) + NORM_EPS)
        xh = x * r
        t = dn * xh
        dg_ref[...] += jnp.sum(t.reshape(cnt // 8, 8, HD), axis=0)
        dng = dn * gain
        return (r * (dng - xh * jnp.mean(dng * xh, axis=-1, keepdims=True))).astype(BF16)

    for qb in reversed(range(n_pos // QB)):
        last = qb == n_pos // QB - 1
        sl = slice(qb * QB, (qb + 1) * QB)
        for head in range(2):
            hs = slice(head * HD, (head + 1) * HD)
            q, dob = rot[sl, hs], d_o[sl, hs]
            ps = softmax_t(k, q, qb)
            dps = [lax.dot_general(v[at:at + p.shape[0]], dob, NT, preferred_element_type=F32) for at, p in ps]
            delta = functools.reduce(jnp.add, [jnp.sum(p * dp, axis=0, keepdims=True) for (_, p), dp in zip(ps, dps)])
            dq_t = None
            for (at, p), dp in zip(ps, dps):
                ds = (p * (dp - delta) * HD ** -0.5).astype(BF16)
                dq_p = jnp.dot(k_t[:, at:at + p.shape[0]], ds, preferred_element_type=F32)
                dq_t = dq_p if dq_t is None else dq_t + dq_p
                dv = jnp.dot(p.astype(BF16), dob, preferred_element_type=F32)
                dk = jnp.dot(ds, q, preferred_element_type=F32)
                rows = pl.ds(at, dk.shape[0])
                if last and head == 0:
                    dk_acc[rows, :] = dk
                    dv_acc[rows, :] = dv
                else:
                    dk_acc[rows, :] += dk
                    dv_acc[rows, :] += dv
            dq_raw = post_back(dq_t.T, raw[sl, hs], gq_ref[...], qb * QB, dgq_ref)
            oq_ref[pl.ds(qb * src_b, src_b), 0, :, pl.ds(head * HD, HD)] = dq_raw.reshape(src_b, tok, HD)
    dk_raw = post_back(dk_acc[...], raw[:, 2 * HD:], gk_ref[...], 0, dgk_ref)
    ok_ref[:, 0] = dk_raw.reshape(n_src, tok, HD)
    ov_ref[:, 0] = dv_acc[...].astype(BF16).reshape(n_src, tok, HD)


def dx_kernel(dq_ref, dk_ref, dv_ref, wq_ref, wk_ref, wv_ref, x_ref, dy_ref, g_ref, dx_ref, dg_ref):
    n_src, rows, tok, dim = x_ref.shape
    n = n_src * rows * tok

    @pl.when(pl.program_id(0) == 0)
    def _():
        dg_ref[...] = jnp.zeros_like(dg_ref)

    dn = functools.reduce(jnp.add, [
        lax.dot_general(d[...].reshape(n, d.shape[-1]), w[...], NT, preferred_element_type=F32)
        for d, w in ((dq_ref, wq_ref), (dk_ref, wk_ref), (dv_ref, wv_ref))])
    x = x_ref[...].reshape(n, dim).astype(F32)
    r = lax.rsqrt(jnp.mean(x * x, axis=-1, keepdims=True) + NORM_EPS)
    xh = x * r
    dg_ref[...] += jnp.sum((dn * xh).reshape(n // 8, 8, dim), axis=0)
    dng = dn * g_ref[...]
    dx = r * (dng - xh * jnp.mean(dng * xh, axis=-1, keepdims=True))
    dx_ref[...] = (dy_ref[...].reshape(n, dim).astype(F32) + dx).astype(BF16).reshape(dx_ref.shape)


MESH = pl.DeviceIdType.MESH


def tail_kernel(n_dev, *refs):
    wq, wk, wv, dx, gains, oq, ok, ov, odx, ogains = refs[:10]
    chunks = [(wq, oq, 0, wq.shape[0] // 2), (wq, oq, wq.shape[0] // 2, wq.shape[0] // 2), (wk, ok, 0, wk.shape[0]), (wv, ov, 0, wv.shape[0])]
    nc = len(chunks)
    acc, r1, r2, r3 = (refs[10 + i * nc:10 + (i + 1) * nc] for i in range(4))
    gbuf, xbuf, send, recv, loc, xsend, xrecv, gsend, grecv, lsem = refs[10 + 4 * nc:]
    me = lax.axis_index('sp')
    c, x, y = me % 2, (me // 2) % 2, me // 4
    pn, xn, yn = me + 1 - 2 * c, me + 2 - 4 * x, me + 4 - 8 * y
    peers = [(me + d) % n_dev for d in range(1, n_dev)]

    barrier = pltpu.get_barrier_semaphore()
    for p in peers:
        pl.semaphore_signal(barrier, inc=1, device_id=(p,), device_id_type=MESH)
    pl.semaphore_wait(barrier, n_dev - 1)

    def rdma(src, dst, ci, slot, dev):
        return pltpu.make_async_remote_copy(src_ref=src, dst_ref=dst, send_sem=send.at[ci, slot], recv_sem=recv.at[ci, slot],
                                            device_id=(dev,), device_id_type=MESH)

    def add(dst, d0, src, s0, n):
        step = 8
        def body(i, _):
            dst[pl.ds(pl.multiple_of(d0 + i * step, 8), step), :] += src[pl.ds(pl.multiple_of(s0 + i * step, 8), step), :]
            return 0
        lax.fori_loop(0, n // step, body, 0, unroll=2)

    started = []

    def go(copies):
        for cp in copies:
            cp.start()
        started.extend(copies)
        return copies

    flight = {}

    def s1(i):
        src, out, row0, n = chunks[i]
        half = n // 2
        mine = pltpu.make_async_copy(src.at[pl.ds(pl.multiple_of(row0 + c * half, 8), half), :], acc[i], loc.at[i, 0])
        mine.start()
        flight[i, 1] = (mine, go([rdma(src.at[pl.ds(pl.multiple_of(row0 + (1 - c) * half, 8), half), :], r1[i], i, 0, pn)]))

    def s2(i):
        n = chunks[i][3]
        mine, cps = flight[i, 1]
        mine.wait()
        cps[0].wait_recv()
        add(acc[i], 0, r1[i], 0, n // 2)
        e = n // 8
        flight[i, 2] = go([rdma(acc[i].at[pl.ds(pl.multiple_of((1 - x) * e, 8), e), :], r2[i].at[0], i, 1, xn),
                           rdma(acc[i].at[pl.ds(pl.multiple_of(n // 4 + (1 - y) * e, 8), e), :], r2[i].at[1], i, 2, yn)])

    def s3(i):
        n = chunks[i][3]
        e, f = n // 8, n // 16
        for cp in flight[i, 2]:
            cp.wait_recv()
        p1, q1 = x * e, n // 4 + y * e
        add(acc[i], p1, r2[i].at[0], 0, e)
        add(acc[i], q1, r2[i].at[1], 0, e)
        flight[i, 3] = go([rdma(acc[i].at[pl.ds(pl.multiple_of(p1 + (1 - y) * f, 8), f), :], r3[i].at[0], i, 3, yn),
                           rdma(acc[i].at[pl.ds(pl.multiple_of(q1 + (1 - x) * f, 8), f), :], r3[i].at[1], i, 4, xn)])

    def s4(i):
        _, out, row0, n = chunks[i]
        e, f = n // 8, n // 16
        for cp in flight[i, 3]:
            cp.wait_recv()
        p, q = x * e + y * f, n // 4 + y * e + x * f
        add(acc[i], p, r3[i].at[0], 0, f)
        add(acc[i], q, r3[i].at[1], 0, f)
        base = row0 + c * (n // 2)
        ps, qs = acc[i].at[pl.ds(pl.multiple_of(p, 8), f), :], acc[i].at[pl.ds(pl.multiple_of(q, 8), f), :]
        po, qo = out.at[pl.ds(pl.multiple_of(base + p, 8), f), :], out.at[pl.ds(pl.multiple_of(base + q, 8), f), :]
        mine = [pltpu.make_async_copy(ps, po, loc.at[i, 1]), pltpu.make_async_copy(qs, qo, loc.at[i, 2])]
        for cp in mine:
            cp.start()
        flight[i, 4] = (mine, go([rdma(ps, po, i, 5, yn), rdma(qs, qo, i, 6, xn), rdma(ps, po, i, 7, xn), rdma(qs, qo, i, 8, yn)]))

    def s5(i):
        _, out, row0, n = chunks[i]
        e, f = n // 8, n // 16
        cps = flight[i, 4][1]
        cps[0].wait_recv()
        cps[1].wait_recv()
        base = row0 + c * (n // 2)
        po = out.at[pl.ds(pl.multiple_of(base + x * e + (1 - y) * f, 8), f), :]
        qo = out.at[pl.ds(pl.multiple_of(base + n // 4 + y * e + (1 - x) * f, 8), f), :]
        flight[i, 5] = go([rdma(po, po, i, 9, xn), rdma(qo, qo, i, 10, yn)])

    def s6(i):
        _, out, row0, n = chunks[i]
        mine, cps = flight[i, 4]
        for cp in mine:
            cp.wait()
        for cp in (cps[2], cps[3], *flight[i, 5]):
            cp.wait_recv()
        rows = out.at[pl.ds(pl.multiple_of(row0 + c * (n // 2), 8), n // 2), :]
        flight[i, 6] = go([rdma(rows, rows, i, 11, pn)])

    rows = dx.shape[1]

    def send_dx(d):
        to = me + (1 - 2 * c) * (d % 2) + (2 - 4 * x) * ((d // 2) % 2) + (4 - 8 * y) * (d // 4)
        cp = pltpu.make_async_remote_copy(src_ref=dx.at[to], dst_ref=odx.at[pl.ds(pl.multiple_of(me * rows, rows), rows)],
                                          send_sem=xsend.at[d], recv_sem=xrecv.at[d], device_id=(to,), device_id_type=MESH)
        cp.start()
        return cp

    for i in range(nc):
        s1(i)
    gcopies = []
    for d in range(1, n_dev):
        cp = pltpu.make_async_remote_copy(src_ref=gains, dst_ref=gbuf.at[d - 1], send_sem=gsend.at[d], recv_sem=grecv.at[d],
                                          device_id=(peers[d - 1],), device_id_type=MESH)
        cp.start()
        gcopies.append(cp)
    keep_in = pltpu.make_async_copy(dx.at[me], xbuf, lsem.at[0])
    keep_in.start()
    xcopies = [send_dx(d) for d in (2, 4, 1)]
    filler = [3, 5, 6, 7]
    stages = [s2, s3, s4, s5, s6]
    keep_out = None
    for t in range(nc + len(stages) - 1):
        for k in reversed(range(len(stages))):
            if 0 <= t - k < nc:
                stages[k](t - k)
        if t >= 2 and filler:
            xcopies.append(send_dx(filler.pop(0)))
        if t == 1:
            keep_in.wait()
            keep_out = pltpu.make_async_copy(xbuf, odx.at[pl.ds(pl.multiple_of(me * rows, rows), rows)], lsem.at[1])
            keep_out.start()
    for cp in gcopies:
        cp.wait()
    ogains[...] = gains[...] + functools.reduce(jnp.add, [gbuf[d] for d in range(n_dev - 1)])
    keep_out.wait()
    for i in range(nc):
        flight[i, 6][0].wait_recv()
    for cp in started:
        cp.wait_send()
    for cp in xcopies:
        cp.wait()


def finish(n_dev, dwq, dwk, dwv, dx, gains):
    nd, rows, tok, dim = dx.shape
    hbm, vmem = pl.BlockSpec(memory_space=pl.ANY), pl.BlockSpec(memory_space=pltpu.VMEM)
    sizes = [(dwq.shape[0] // 2, dwq.shape[1])] * 2 + [dwk.shape, dwv.shape]
    nc = len(sizes)
    dma = pltpu.SemaphoreType.DMA
    scratch = [pltpu.VMEM((r // 2, w), F32) for r, w in sizes] + [pltpu.VMEM((r // 2, w), F32) for r, w in sizes]
    scratch += [pltpu.VMEM((2, r // 8, w), F32) for r, w in sizes] + [pltpu.VMEM((2, r // 16, w), F32) for r, w in sizes]
    scratch += [pltpu.VMEM((n_dev - 1,) + gains.shape, F32), pltpu.VMEM((rows, tok, dim), BF16)]
    scratch += [dma((nc, 12)), dma((nc, 12)), dma((nc, 3)), dma((n_dev,)), dma((n_dev,)), dma((n_dev,)), dma((n_dev,)), dma((2,))]
    return pl.pallas_call(
        functools.partial(tail_kernel, n_dev), in_specs=[hbm] * 4 + [vmem], out_specs=[hbm] * 4 + [vmem],
        out_shape=[jax.ShapeDtypeStruct(a.shape, F32) for a in (dwq, dwk, dwv)] + [
            jax.ShapeDtypeStruct((nd * rows, tok, dim), BF16), jax.ShapeDtypeStruct(gains.shape, F32)],
        scratch_shapes=scratch, compiler_params=params(collective_id=0, has_side_effects=True), name='tail',
    )(dwq, dwk, dwv, dx, gains)


def params(**kw):
    return pltpu.CompilerParams(vmem_limit_bytes=VMEM_LIMIT, **kw)


def cost(flops, nbytes):
    return pl.CostEstimate(flops=int(flops), bytes_accessed=int(nbytes), transcendentals=0)


def solution(mesh):
    n_dev = mesh.shape['sp']
    seq_spec = P(None, 'sp', None)
    replicated = P()

    def local_step(hidden, norm_gain, w_q, w_k, w_v, q_gain, k_gain, w_o, d_out):
        n_batch, tok, dim = hidden.shape
        rows = n_batch // n_dev
        n_pos = tok * n_dev
        n_tok = n_pos * rows
        n_q, n_kv = w_q.shape[1] // HD, w_k.shape[1] // HD
        qw = n_q * HD
        cos_t, sin_t = rope_tables(n_pos)
        g2 = norm_gain.reshape(1, dim)
        gq2, gk2 = q_gain.reshape(1, HD), k_gain.reshape(1, HD)
        x = lax.all_to_all(hidden, 'sp', 0, 0, tiled=True).reshape(n_dev, rows, tok, dim)
        dy = lax.all_to_all(d_out, 'sp', 0, 0, tiled=True).reshape(n_dev, rows, tok, dim)

        sb = 2
        full = lambda *s: pl.BlockSpec(s, lambda *i: (0,) * len(s))
        tokspec = lambda c: pl.BlockSpec((sb, rows, tok, c), lambda i: (i, 0, 0, 0))
        shp = lambda c, d=BF16: jax.ShapeDtypeStruct((n_dev, rows, tok, c), d)
        h, raw, rot = pl.pallas_call(
            qkv_kernel, grid=(n_dev // sb,),
            in_specs=[tokspec(dim), full(1, dim), full(*w_q.shape), full(*w_k.shape), full(*w_v.shape), full(1, HD), full(1, HD),
                      pl.BlockSpec((sb * tok, HD), lambda i: (i, 0)), pl.BlockSpec((sb * tok, HD), lambda i: (i, 0))],
            out_specs=[tokspec(dim), tokspec(n_kv * 3 * HD), tokspec(n_kv * 4 * HD)],
            out_shape=[shp(dim), shp(n_kv * 3 * HD), shp(n_kv * 4 * HD)],
            compiler_params=params(), cost_estimate=cost(2 * n_tok * dim * 4 * HD * n_kv, 40e6), name='qkv',
        )(x, g2, w_q, w_k, w_v, gq2, gk2, cos_t, sin_t)

        head_spec = lambda c: pl.BlockSpec((n_dev, 1, tok, c), lambda r, j: (0, r, 0, j))
        o = pl.pallas_call(
            attn_fwd_kernel, grid=(rows, n_kv), in_specs=[head_spec(4 * HD)], out_specs=head_spec(2 * HD),
            out_shape=shp(qw), compiler_params=params(), cost_estimate=cost(4 * n_tok * n_pos * qw, 24e6), name='attn_fwd',
        )(rot)
        o2, dy2, x2 = o.reshape(n_tok, qw), dy.reshape(n_tok, dim), x.reshape(n_tok, dim)
        y = (x2.astype(F32) + jnp.dot(o2, w_o, preferred_element_type=F32)).astype(BF16)
        d_wo = lax.dot_general(o2, dy2, (((0,), (0,)), ((), ())), preferred_element_type=F32)
        d_o = lax.dot_general(dy2, w_o, (((1,), (1,)), ((), ())), preferred_element_type=F32).astype(BF16).reshape(n_dev, rows, tok, qw)
        y, d_wo, d_o = lax.optimization_barrier((y, d_wo, d_o))
        y_out = lax.all_to_all(y.reshape(n_batch, tok, dim), 'sp', 0, 0, tiled=True)

        dq, dk, dv, dgq, dgk = pl.pallas_call(
            attn_bwd_kernel, grid=(rows, n_kv),
            in_specs=[head_spec(4 * HD), head_spec(3 * HD), head_spec(2 * HD), full(1, HD), full(1, HD), full(n_pos, HD), full(n_pos, HD)],
            out_specs=[head_spec(2 * HD), head_spec(HD), head_spec(HD), full(8, HD), full(8, HD)],
            out_shape=[shp(qw), shp(n_kv * HD), shp(n_kv * HD), jax.ShapeDtypeStruct((8, HD), F32), jax.ShapeDtypeStruct((8, HD), F32)],
            scratch_shapes=[pltpu.VMEM((n_pos, HD), F32), pltpu.VMEM((n_pos, HD), F32)],
            compiler_params=params(), cost_estimate=cost(10 * n_tok * n_pos * qw, 60e6), name='attn_bwd',
        )(rot, raw, d_o, gq2, gk2, cos_t, sin_t)

        dq, y_out = lax.optimization_barrier((dq, y_out))
        h2 = h.reshape(n_tok, dim)
        d_wq, d_wk, d_wv = (lax.dot_general(h2, d.reshape(n_tok, -1), (((0,), (0,)), ((), ())), preferred_element_type=F32) for d in (dq, dk, dv))
        dx, dg = pl.pallas_call(
            dx_kernel, grid=(n_dev // sb,),
            in_specs=[tokspec(qw), tokspec(n_kv * HD), tokspec(n_kv * HD), full(*w_q.shape), full(*w_k.shape), full(*w_v.shape), tokspec(dim), tokspec(dim), full(1, dim)],
            out_specs=[tokspec(dim), full(8, dim)],
            out_shape=[shp(dim), jax.ShapeDtypeStruct((8, dim), F32)],
            compiler_params=params(), cost_estimate=cost(2 * n_tok * dim * 4 * HD * n_kv, 40e6), name='dx',
        )(dq, dk, dv, w_q, w_k, w_v, x, dy, g2)
        d_wo = lax.psum(d_wo, 'sp')
        gains = jnp.concatenate([jnp.sum(dg, 0), jnp.sum(dgq, 0), jnp.sum(dgk, 0)])
        gains = jnp.pad(gains, (0, -gains.size % 1024)).reshape(-1, 128)
        d_wq, d_wk, d_wv, d_hidden, gains = finish(n_dev, d_wq, d_wk, d_wv, dx, gains)
        gains = gains.reshape(-1)
        return (y_out, d_hidden, d_wq, d_wk, d_wv, d_wo, gains[:dim], gains[dim:dim + HD], gains[dim + HD:dim + 2 * HD])

    return jax.shard_map(local_step, mesh=mesh, in_specs=(seq_spec,) + (replicated,) * 7 + (seq_spec,),
                         out_specs=(seq_spec, seq_spec) + (replicated,) * 7, check_vma=False)
```

```python
import math
import functools
import jax
import jax.numpy as jnp
from jax import lax
from jax.experimental import pallas as pl
from jax.experimental.pallas import tpu as pltpu
from jax.sharding import PartitionSpec as P

ROPE_BASE = 1000000.0
NORM_EPS = 1e-6
F32 = jnp.float32
BF16 = jnp.bfloat16
HD = 128
VMEM_LIMIT = 60 * 1024 * 1024


def rope_tables(n_pos):
    half = HD // 2
    inv_freq = jnp.exp(jnp.arange(half).astype(F32) * (-2.0 * math.log(ROPE_BASE) / HD))
    angles = jnp.arange(n_pos).astype(F32)[:, None] * inv_freq[None, :]
    cos, sin = jnp.cos(angles), jnp.sin(angles)
    return jnp.concatenate([cos, cos], axis=-1), jnp.concatenate([-sin, sin], axis=-1)


def qkv_kernel(x_ref, g_ref, wq_ref, wk_ref, wv_ref, gq_ref, gk_ref, cos_ref, sin_ref, h_ref, raw_ref, rot_ref):
    n_src, rows, tok, dim = x_ref.shape
    n = n_src * rows * tok
    x = x_ref[...].reshape(n, dim).astype(F32)
    r = lax.rsqrt(jnp.mean(x * x, axis=-1, keepdims=True) + NORM_EPS)
    h_ref[...] = (x * r * g_ref[...]).astype(BF16).reshape(h_ref.shape)
    cos = cos_ref[...].reshape(n_src, 1, tok, HD)
    sin = sin_ref[...].reshape(n_src, 1, tok, HD)

    def post(raw, gain):
        v = raw.astype(F32)
        v = v * lax.rsqrt(jnp.mean(v * v, axis=-1, keepdims=True) + NORM_EPS) * gain
        rolled = pltpu.roll(v, HD // 2, 1).reshape(n_src, rows, tok, HD)
        return (v.reshape(n_src, rows, tok, HD) * cos + rolled * sin).astype(BF16)

    gq, gk = gq_ref[...], gk_ref[...]
    shape = (n_src, rows, tok, HD)

    def body(j, _):
        hh = h_ref[...].reshape(n, dim)

        def proj(w_ref, width):
            cols = pl.ds(pl.multiple_of(j * width, width), width)
            return jnp.dot(hh, w_ref[:, cols], preferred_element_type=F32).astype(BF16)

        q, k, v = proj(wq_ref, 4 * HD), proj(wk_ref, 2 * HD), proj(wv_ref, 2 * HD)
        for i in range(2):
            heads = [q[:, 2 * i * HD:(2 * i + 1) * HD], q[:, (2 * i + 1) * HD:(2 * i + 2) * HD], k[:, i * HD:(i + 1) * HD]]
            for part, (val, gain) in enumerate(zip(heads, (gq, gq, gk))):
                raw_ref[:, :, :, pl.ds(pl.multiple_of((2 * j + i) * 3 * HD + part * HD, HD), HD)] = val.reshape(shape)
                rot_ref[:, :, :, pl.ds(pl.multiple_of((2 * j + i) * 4 * HD + part * HD, HD), HD)] = post(val, gain)
            rot_ref[:, :, :, pl.ds(pl.multiple_of((2 * j + i) * 4 * HD + 3 * HD, HD), HD)] = v[:, i * HD:(i + 1) * HD].reshape(shape)
        return 0

    lax.fori_loop(0, wk_ref.shape[1] // (2 * HD), body, 0, unroll=2)


QB = 256
NT = (((1,), (1,)), ((), ()))
EXP_SCALE = HD ** -0.5 * math.log2(math.e)


def softmax_t(k, q, qb):
    lo = qb * QB
    parts = [(lo, lax.dot_general(k[lo:lo + QB], q, NT, preferred_element_type=F32))]
    keys = lax.broadcasted_iota(jnp.int32, (QB, QB), 0)
    queries = lax.broadcasted_iota(jnp.int32, (QB, QB), 1)
    parts[0] = (lo, jnp.where(keys <= queries, parts[0][1], -1e30))
    if lo:
        parts.append((0, lax.dot_general(k[:lo], q, NT, preferred_element_type=F32)))
    top = functools.reduce(jnp.maximum, [jnp.max(s, axis=0, keepdims=True) for _, s in parts])
    exps = [(at, jnp.exp2((s - top) * EXP_SCALE)) for at, s in parts]
    inv = 1.0 / functools.reduce(jnp.add, [jnp.sum(e, axis=0, keepdims=True) for _, e in exps])
    return [(at, e * inv) for at, e in exps]


def attn_fwd_kernel(rot_ref, o_ref):
    n_pos = rot_ref.shape[0] * rot_ref.shape[2]
    rot = rot_ref[...].reshape(n_pos, 4 * HD)
    k, v_t = rot[:, 2 * HD:3 * HD], rot[:, 3 * HD:].T
    src_b = QB // rot_ref.shape[2]
    for qb in range(n_pos // QB):
        for head in range(2):
            q = rot[qb * QB:(qb + 1) * QB, head * HD:(head + 1) * HD]
            o_t = functools.reduce(jnp.add, [
                jnp.dot(v_t[:, at:at + p.shape[0]], p.astype(BF16), preferred_element_type=F32)
                for at, p in softmax_t(k, q, qb)])
            o_ref[pl.ds(qb * src_b, src_b), 0, :, pl.ds(head * HD, HD)] = o_t.T.astype(BF16).reshape(src_b, o_ref.shape[2], HD)


def attn_bwd_kernel(rot_ref, raw_ref, do_ref, gq_ref, gk_ref, cos_ref, sin_ref, oq_ref, ok_ref, ov_ref, dgq_ref, dgk_ref, dk_acc, dv_acc):
    n_src, _, tok, _ = rot_ref.shape
    n_pos = n_src * tok
    rot = rot_ref[...].reshape(n_pos, 4 * HD)
    raw = raw_ref[...].reshape(n_pos, 3 * HD)
    d_o = do_ref[...].reshape(n_pos, 2 * HD)
    k, v = rot[:, 2 * HD:3 * HD], rot[:, 3 * HD:]
    k_t = k.astype(F32).T.astype(BF16)
    src_b = QB // tok
    first = jnp.logical_and(pl.program_id(0) == 0, pl.program_id(1) == 0)

    @pl.when(first)
    def _():
        dgq_ref[...] = jnp.zeros_like(dgq_ref)
        dgk_ref[...] = jnp.zeros_like(dgk_ref)

    def post_back(d, x_raw, gain, lo, dg_ref):
        cnt = d.shape[0]
        d = d.astype(BF16).astype(F32)
        c, s = cos_ref[pl.ds(lo, cnt), :], sin_ref[pl.ds(lo, cnt), :]
        dn = d * c + pltpu.roll(d * s, HD // 2, 1)
        x = x_raw.astype(F32)
        r = lax.rsqrt(jnp.mean(x * x, axis=-1, keepdims=True) + NORM_EPS)
        xh = x * r
        t = dn * xh
        dg_ref[...] += jnp.sum(t.reshape(cnt // 8, 8, HD), axis=0)
        dng = dn * gain
        return (r * (dng - xh * jnp.mean(dng * xh, axis=-1, keepdims=True))).astype(BF16)

    for qb in reversed(range(n_pos // QB)):
        last = qb == n_pos // QB - 1
        sl = slice(qb * QB, (qb + 1) * QB)
        for head in range(2):
            hs = slice(head * HD, (head + 1) * HD)
            q, dob = rot[sl, hs], d_o[sl, hs]
            ps = softmax_t(k, q, qb)
            dps = [lax.dot_general(v[at:at + p.shape[0]], dob, NT, preferred_element_type=F32) for at, p in ps]
            delta = functools.reduce(jnp.add, [jnp.sum(p * dp, axis=0, keepdims=True) for (_, p), dp in zip(ps, dps)])
            dq_t = None
            for (at, p), dp in zip(ps, dps):
                ds = (p * (dp - delta) * HD ** -0.5).astype(BF16)
                dq_p = jnp.dot(k_t[:, at:at + p.shape[0]], ds, preferred_element_type=F32)
                dq_t = dq_p if dq_t is None else dq_t + dq_p
                dv = jnp.dot(p.astype(BF16), dob, preferred_element_type=F32)
                dk = jnp.dot(ds, q, preferred_element_type=F32)
                rows = pl.ds(at, dk.shape[0])
                if last and head == 0:
                    dk_acc[rows, :] = dk
                    dv_acc[rows, :] = dv
                else:
                    dk_acc[rows, :] += dk
                    dv_acc[rows, :] += dv
            dq_raw = post_back(dq_t.T, raw[sl, hs], gq_ref[...], qb * QB, dgq_ref)
            oq_ref[pl.ds(qb * src_b, src_b), 0, :, pl.ds(head * HD, HD)] = dq_raw.reshape(src_b, tok, HD)
    dk_raw = post_back(dk_acc[...], raw[:, 2 * HD:], gk_ref[...], 0, dgk_ref)
    ok_ref[:, 0] = dk_raw.reshape(n_src, tok, HD)
    ov_ref[:, 0] = dv_acc[...].astype(BF16).reshape(n_src, tok, HD)


MESH = pl.DeviceIdType.MESH


def tail_kernel(n_dev, *refs):
    wq, wk, wv, dq, dk, dv, pq, pk, pv, x_hbm, dy_hbm, g_ref, dgq, dgk, oq, ok, ov, odx, ogains = refs[:19]
    chunks = [(wk, ok, 0, wk.shape[0]), (wv, ov, 0, wv.shape[0]), (wq, oq, 0, wq.shape[0] // 2), (wq, oq, wq.shape[0] // 2, wq.shape[0] // 2)]
    nc = len(chunks)
    acc, r1, r2, r3 = (refs[19 + i * nc:19 + (i + 1) * nc] for i in range(4))
    (vq, vk, vv, bq, bk, bv, bx, by, dn, dxb, gpack, gbuf,
     send, recv, loc, xsend, xrecv, gsend, grecv, lsem, wsem, bsem) = refs[19 + 4 * nc:]
    me = lax.axis_index('sp')
    c, x, y = me % 2, (me // 2) % 2, me // 4
    pn, xn, yn = me + 1 - 2 * c, me + 2 - 4 * x, me + 4 - 8 * y
    peers = [(me + d) % n_dev for d in range(1, n_dev)]

    barrier = pltpu.get_barrier_semaphore()
    for p in peers:
        pl.semaphore_signal(barrier, inc=1, device_id=(p,), device_id_type=MESH)
    pl.semaphore_wait(barrier, n_dev - 1)

    def rdma(src, dst, ci, slot, dev):
        return pltpu.make_async_remote_copy(src_ref=src, dst_ref=dst, send_sem=send.at[ci, slot], recv_sem=recv.at[ci, slot],
                                            device_id=(dev,), device_id_type=MESH)

    def add(dst, d0, src, s0, n):
        step = 8

        def body(i, _):
            dst[pl.ds(pl.multiple_of(d0 + i * step, 8), step), :] += src[pl.ds(pl.multiple_of(s0 + i * step, 8), step), :]
            return 0

        lax.fori_loop(0, n // step, body, 0, unroll=2)

    started = []

    def go(copies):
        for cp in copies:
            cp.start()
        started.extend(copies)
        return copies

    flight = {}

    def s1(i):
        src, _, row0, n = chunks[i]
        half = n // 2
        mine = pltpu.make_async_copy(src.at[pl.ds(pl.multiple_of(row0 + c * half, 8), half), :], acc[i], loc.at[i, 0])
        mine.start()
        flight[i, 1] = (mine, go([rdma(src.at[pl.ds(pl.multiple_of(row0 + (1 - c) * half, 8), half), :], r1[i], i, 0, pn)]))

    def s2(i):
        n = chunks[i][3]
        mine, cps = flight[i, 1]
        mine.wait()
        cps[0].wait_recv()
        add(acc[i], 0, r1[i], 0, n // 2)
        e = n // 8
        flight[i, 2] = go([rdma(acc[i].at[pl.ds(pl.multiple_of((1 - x) * e, 8), e), :], r2[i].at[0], i, 1, xn),
                           rdma(acc[i].at[pl.ds(pl.multiple_of(n // 4 + (1 - y) * e, 8), e), :], r2[i].at[1], i, 2, yn)])

    def s3(i):
        n = chunks[i][3]
        e, f = n // 8, n // 16
        for cp in flight[i, 2]:
            cp.wait_recv()
        p1, q1 = x * e, n // 4 + y * e
        add(acc[i], p1, r2[i].at[0], 0, e)
        add(acc[i], q1, r2[i].at[1], 0, e)
        flight[i, 3] = go([rdma(acc[i].at[pl.ds(pl.multiple_of(p1 + (1 - y) * f, 8), f), :], r3[i].at[0], i, 3, yn),
                           rdma(acc[i].at[pl.ds(pl.multiple_of(q1 + (1 - x) * f, 8), f), :], r3[i].at[1], i, 4, xn)])

    def s4(i):
        _, out, row0, n = chunks[i]
        e, f = n // 8, n // 16
        for cp in flight[i, 3]:
            cp.wait_recv()
        p, q = x * e + y * f, n // 4 + y * e + x * f
        add(acc[i], p, r3[i].at[0], 0, f)
        add(acc[i], q, r3[i].at[1], 0, f)
        base = row0 + c * (n // 2)
        ps, qs = acc[i].at[pl.ds(pl.multiple_of(p, 8), f), :], acc[i].at[pl.ds(pl.multiple_of(q, 8), f), :]
        po, qo = out.at[pl.ds(pl.multiple_of(base + p, 8), f), :], out.at[pl.ds(pl.multiple_of(base + q, 8), f), :]
        mine = [pltpu.make_async_copy(ps, po, loc.at[i, 1]), pltpu.make_async_copy(qs, qo, loc.at[i, 2])]
        for cp in mine:
            cp.start()
        flight[i, 4] = (mine, go([rdma(ps, po, i, 5, yn), rdma(qs, qo, i, 6, xn), rdma(ps, po, i, 7, xn), rdma(qs, qo, i, 8, yn)]))

    def s5(i):
        _, out, row0, n = chunks[i]
        e, f = n // 8, n // 16
        cps = flight[i, 4][1]
        cps[0].wait_recv()
        cps[1].wait_recv()
        base = row0 + c * (n // 2)
        po = out.at[pl.ds(pl.multiple_of(base + x * e + (1 - y) * f, 8), f), :]
        qo = out.at[pl.ds(pl.multiple_of(base + n // 4 + y * e + (1 - x) * f, 8), f), :]
        flight[i, 5] = go([rdma(po, po, i, 9, xn), rdma(qo, qo, i, 10, yn)])

    def s6(i):
        _, out, row0, n = chunks[i]
        mine, cps = flight[i, 4]
        for cp in mine:
            cp.wait()
        for cp in (cps[2], cps[3], *flight[i, 5]):
            cp.wait_recv()
        rows = out.at[pl.ds(pl.multiple_of(row0 + c * (n // 2), 8), n // 2), :]
        flight[i, 6] = go([rdma(rows, rows, i, 11, pn)])

    _, rows, tok, dim = x_hbm.shape
    sb = bx.shape[1]
    n_blk = n_dev // sb
    ntok = sb * rows * tok
    loads = [pltpu.make_async_copy(a, b, wsem.at[i]) for i, (a, b) in enumerate(((pq, vq), (pk, vk), (pv, vv)))]
    order = [(2 - 4 * x) // sb, (4 - 8 * y) // sb, (2 - 4 * x + 4 - 8 * y) // sb, 0]
    blocks = [me // sb + o for o in order]

    def fetch(b):
        src = pl.ds(pl.multiple_of(blocks[b] * sb, sb), sb)
        cps = [pltpu.make_async_copy(a.at[src], v.at[b % 2], bsem.at[b % 2, i])
               for i, (a, v) in enumerate(((dq, bq), (dk, bk), (dv, bv), (x_hbm, bx), (dy_hbm, by)))]
        for cp in cps:
            cp.start()
        return cps

    xcopies = []
    local_out = []

    def dx_block(b, fetched):
        for cp in fetched:
            cp.wait()

        def col(j, _):
            cols = pl.ds(pl.multiple_of(j * 256, 256), 256)
            dn[:, cols] = functools.reduce(jnp.add, [
                lax.dot_general(d[b % 2].reshape(ntok, d.shape[-1]), w[cols, :], NT, preferred_element_type=F32)
                for d, w in ((bq, vq), (bk, vk), (bv, vv))])
            return 0

        lax.fori_loop(0, dim // 256, col, 0)

        def tail_rows(j, _):
            part = pl.ds(pl.multiple_of(j * tok, tok), tok)
            si, ri = j // rows, j % rows
            d = dn[part, :]
            xv = bx[b % 2, si, ri].astype(F32)
            r = lax.rsqrt(jnp.mean(xv * xv, axis=-1, keepdims=True) + NORM_EPS)
            xh = xv * r
            gpack[:, pl.ds(0, dim)] += jnp.sum((d * xh).reshape(tok // 8, 8, dim), axis=0)
            dng = d * g_ref[...]
            dx = r * (dng - xh * jnp.mean(dng * xh, axis=-1, keepdims=True))
            dxb[b, si, ri] = (by[b % 2, si, ri].astype(F32) + dx).astype(BF16)
            return 0

        lax.fori_loop(0, sb * rows, tail_rows, 0)
        home = odx.at[pl.ds(pl.multiple_of(me * rows, rows), rows)]
        for si in range(sb):
            core = (c + si) % 2
            to = blocks[b] * sb + core
            if b == n_blk - 1 and si == 0:
                cp = pltpu.make_async_copy(dxb.at[b, core], home, lsem.at[0])
                local_out.append(cp)
            else:
                cp = pltpu.make_async_remote_copy(src_ref=dxb.at[b, core], dst_ref=home, send_sem=xsend.at[b, si], recv_sem=xrecv.at[b, si],
                                                  device_id=(to,), device_id_type=MESH)
                xcopies.append(cp)
            cp.start()

    for i in range(nc):
        s1(i)
    for cp in loads:
        cp.start()
    fetched = {0: fetch(0)}
    gpack[:, pl.ds(0, dim)] = jnp.zeros((8, dim), F32)
    gpack[:, pl.ds(dim, HD)] = dgq[...]
    gpack[:, pl.ds(dim + HD, HD)] = dgk[...]
    fetched[1] = fetch(1)
    for i in range(nc):
        s2(i)
    for cp in loads:
        cp.wait()
    dx_block(0, fetched[0])
    fetched[2] = fetch(2)
    s3(0)
    s3(1)
    dx_block(1, fetched[1])
    fetched[3] = fetch(3)
    s4(0)
    s3(2)
    s4(1)
    s3(3)
    dx_block(2, fetched[2])
    s5(0)
    s4(2)
    s5(1)
    s4(3)
    dx_block(3, fetched[3])
    gcopies = []
    for d in range(1, n_dev):
        cp = pltpu.make_async_remote_copy(src_ref=gpack, dst_ref=gbuf.at[d - 1], send_sem=gsend.at[d], recv_sem=grecv.at[d],
                                          device_id=(peers[d - 1],), device_id_type=MESH)
        cp.start()
        gcopies.append(cp)
    s6(0)
    s5(2)
    s6(1)
    s5(3)
    s6(2)
    s6(3)
    for cp in gcopies:
        cp.wait()
    total = gpack[...] + functools.reduce(jnp.add, [gbuf[d] for d in range(n_dev - 1)])
    ogains[...] = jnp.sum(total, axis=0, keepdims=True)
    for cp in local_out:
        cp.wait()
    for i in range(nc):
        flight[i, 6][0].wait_recv()
    for cp in started:
        cp.wait_send()
    for cp in xcopies:
        cp.wait()


def finish(n_dev, parts, d_parts, weights, x, dy, g2, dgq, dgk):
    dwq, dwk, dwv = parts
    nd, rows, tok, dim = x.shape
    sb = 2
    hbm, vmem = pl.BlockSpec(memory_space=pl.ANY), pl.BlockSpec(memory_space=pltpu.VMEM)
    sizes = [dwk.shape, dwv.shape] + [(dwq.shape[0] // 2, dwq.shape[1])] * 2
    nc = len(sizes)
    dma = pltpu.SemaphoreType.DMA
    scratch = [pltpu.VMEM((r // 2, w), F32) for r, w in sizes] + [pltpu.VMEM((r // 2, w), F32) for r, w in sizes]
    scratch += [pltpu.VMEM((2, r // 8, w), F32) for r, w in sizes] + [pltpu.VMEM((2, r // 16, w), F32) for r, w in sizes]
    scratch += [pltpu.VMEM(w.shape, BF16) for w in weights]
    scratch += [pltpu.VMEM((2, sb, rows, tok, d.shape[-1]), BF16) for d in (*d_parts, x, dy)]
    scratch += [pltpu.VMEM((sb * rows * tok, dim), F32), pltpu.VMEM((nd // sb, sb, rows, tok, dim), BF16)]
    scratch += [pltpu.VMEM((8, dim + 2 * HD), F32), pltpu.VMEM((n_dev - 1, 8, dim + 2 * HD), F32)]
    scratch += [dma((nc, 12)), dma((nc, 12)), dma((nc, 3)), dma((nd // sb, sb)), dma((nd // sb, sb)), dma((n_dev,)), dma((n_dev,)), dma((1,)), dma((3,)), dma((2, 5))]
    return pl.pallas_call(
        functools.partial(tail_kernel, n_dev), in_specs=[hbm] * 11 + [vmem] * 3, out_specs=[hbm] * 4 + [vmem],
        out_shape=[jax.ShapeDtypeStruct(a.shape, F32) for a in parts] + [
            jax.ShapeDtypeStruct((nd * rows, tok, dim), BF16), jax.ShapeDtypeStruct((1, dim + 2 * HD), F32)],
        scratch_shapes=scratch, compiler_params=params(collective_id=0, has_side_effects=True), name='tail',
    )(*parts, *d_parts, *weights, x, dy, g2, dgq, dgk)


def params(**kw):
    return pltpu.CompilerParams(vmem_limit_bytes=VMEM_LIMIT, **kw)


def cost(flops, nbytes):
    return pl.CostEstimate(flops=int(flops), bytes_accessed=int(nbytes), transcendentals=0)


def solution(mesh):
    n_dev = mesh.shape['sp']
    seq_spec = P(None, 'sp', None)
    replicated = P()

    def local_step(hidden, norm_gain, w_q, w_k, w_v, q_gain, k_gain, w_o, d_out):
        n_batch, tok, dim = hidden.shape
        rows = n_batch // n_dev
        n_pos = tok * n_dev
        n_tok = n_pos * rows
        n_q, n_kv = w_q.shape[1] // HD, w_k.shape[1] // HD
        qw = n_q * HD
        cos_t, sin_t = rope_tables(n_pos)
        g2 = norm_gain.reshape(1, dim)
        gq2, gk2 = q_gain.reshape(1, HD), k_gain.reshape(1, HD)
        x = lax.all_to_all(hidden, 'sp', 0, 0, tiled=True).reshape(n_dev, rows, tok, dim)
        dy = lax.all_to_all(d_out, 'sp', 0, 0, tiled=True).reshape(n_dev, rows, tok, dim)

        sb = 2
        full = lambda *s: pl.BlockSpec(s, lambda *i: (0,) * len(s))
        tokspec = lambda c: pl.BlockSpec((sb, rows, tok, c), lambda i: (i, 0, 0, 0))
        shp = lambda c, d=BF16: jax.ShapeDtypeStruct((n_dev, rows, tok, c), d)
        h, raw, rot = pl.pallas_call(
            qkv_kernel, grid=(n_dev // sb,),
            in_specs=[tokspec(dim), full(1, dim), full(*w_q.shape), full(*w_k.shape), full(*w_v.shape), full(1, HD), full(1, HD),
                      pl.BlockSpec((sb * tok, HD), lambda i: (i, 0)), pl.BlockSpec((sb * tok, HD), lambda i: (i, 0))],
            out_specs=[tokspec(dim), tokspec(n_kv * 3 * HD), tokspec(n_kv * 4 * HD)],
            out_shape=[shp(dim), shp(n_kv * 3 * HD), shp(n_kv * 4 * HD)],
            compiler_params=params(), cost_estimate=cost(2 * n_tok * dim * 4 * HD * n_kv, 40e6), name='qkv',
        )(x, g2, w_q, w_k, w_v, gq2, gk2, cos_t, sin_t)

        head_spec = lambda c: pl.BlockSpec((n_dev, 1, tok, c), lambda r, j: (0, r, 0, j))
        o = pl.pallas_call(
            attn_fwd_kernel, grid=(rows, n_kv), in_specs=[head_spec(4 * HD)], out_specs=head_spec(2 * HD),
            out_shape=shp(qw), compiler_params=params(), cost_estimate=cost(4 * n_tok * n_pos * qw, 24e6), name='attn_fwd',
        )(rot)
        o2, dy2, x2 = o.reshape(n_tok, qw), dy.reshape(n_tok, dim), x.reshape(n_tok, dim)
        y = (x2.astype(F32) + jnp.dot(o2, w_o, preferred_element_type=F32)).astype(BF16)
        d_wo = lax.dot_general(o2, dy2, (((0,), (0,)), ((), ())), preferred_element_type=F32)
        d_o = lax.dot_general(dy2, w_o, (((1,), (1,)), ((), ())), preferred_element_type=F32).astype(BF16).reshape(n_dev, rows, tok, qw)
        y, d_wo, d_o = lax.optimization_barrier((y, d_wo, d_o))
        y_out = lax.all_to_all(y.reshape(n_batch, tok, dim), 'sp', 0, 0, tiled=True)

        dq, dk, dv, dgq, dgk = pl.pallas_call(
            attn_bwd_kernel, grid=(rows, n_kv),
            in_specs=[head_spec(4 * HD), head_spec(3 * HD), head_spec(2 * HD), full(1, HD), full(1, HD), full(n_pos, HD), full(n_pos, HD)],
            out_specs=[head_spec(2 * HD), head_spec(HD), head_spec(HD), full(8, HD), full(8, HD)],
            out_shape=[shp(qw), shp(n_kv * HD), shp(n_kv * HD), jax.ShapeDtypeStruct((8, HD), F32), jax.ShapeDtypeStruct((8, HD), F32)],
            scratch_shapes=[pltpu.VMEM((n_pos, HD), F32), pltpu.VMEM((n_pos, HD), F32)],
            compiler_params=params(), cost_estimate=cost(10 * n_tok * n_pos * qw, 60e6), name='attn_bwd',
        )(rot, raw, d_o, gq2, gk2, cos_t, sin_t)

        h2 = h.reshape(n_tok, dim)
        d_wq, d_wk, d_wv = (lax.dot_general(h2, d.reshape(n_tok, -1), (((0,), (0,)), ((), ())), preferred_element_type=F32) for d in (dq, dk, dv))
        d_wo = lax.psum(d_wo, 'sp')
        d_wq, d_wk, d_wv, d_hidden, gains = finish(n_dev, (d_wq, d_wk, d_wv), (dq, dk, dv), (w_q, w_k, w_v), x, dy, g2, dgq, dgk)
        gains = gains.reshape(-1)
        return (y_out, d_hidden, d_wq, d_wk, d_wv, d_wo, gains[:dim], gains[dim:dim + HD], gains[dim + HD:dim + 2 * HD])

    return jax.shard_map(local_step, mesh=mesh, in_specs=(seq_spec,) + (replicated,) * 7 + (seq_spec,),
                         out_specs=(seq_spec, seq_spec) + (replicated,) * 7, check_vma=False)
```

```python
import math
import functools
import jax
import jax.numpy as jnp
from jax import lax
from jax.experimental import pallas as pl
from jax.experimental.pallas import tpu as pltpu
from jax.sharding import PartitionSpec as P

ROPE_BASE = 1000000.0
NORM_EPS = 1e-6
F32 = jnp.float32
BF16 = jnp.bfloat16
HD = 128
VMEM_LIMIT = 60 * 1024 * 1024


def rope_tables(n_pos):
    half = HD // 2
    inv_freq = jnp.exp(jnp.arange(half).astype(F32) * (-2.0 * math.log(ROPE_BASE) / HD))
    angles = jnp.arange(n_pos).astype(F32)[:, None] * inv_freq[None, :]
    cos, sin = jnp.cos(angles), jnp.sin(angles)
    return jnp.concatenate([cos, cos], axis=-1), jnp.concatenate([-sin, sin], axis=-1)


def qkv_kernel(x_ref, g_ref, wq_ref, wk_ref, wv_ref, gq_ref, gk_ref, cos_ref, sin_ref, h_ref, raw_ref, rot_ref):
    n_src, rows, tok, dim = x_ref.shape
    n = n_src * rows * tok
    x = x_ref[...].reshape(n, dim).astype(F32)
    r = lax.rsqrt(jnp.mean(x * x, axis=-1, keepdims=True) + NORM_EPS)
    h_ref[...] = (x * r * g_ref[...]).astype(BF16).reshape(h_ref.shape)
    cos = cos_ref[...].reshape(n_src, 1, tok, HD)
    sin = sin_ref[...].reshape(n_src, 1, tok, HD)

    def post(raw, gain):
        v = raw.astype(F32)
        v = v * lax.rsqrt(jnp.mean(v * v, axis=-1, keepdims=True) + NORM_EPS) * gain
        rolled = pltpu.roll(v, HD // 2, 1).reshape(n_src, rows, tok, HD)
        return (v.reshape(n_src, rows, tok, HD) * cos + rolled * sin).astype(BF16)

    gq, gk = gq_ref[...], gk_ref[...]
    shape = (n_src, rows, tok, HD)

    def body(j, _):
        hh = h_ref[...].reshape(n, dim)

        def proj(w_ref, width):
            cols = pl.ds(pl.multiple_of(j * width, width), width)
            return jnp.dot(hh, w_ref[:, cols], preferred_element_type=F32).astype(BF16)

        q, k, v = proj(wq_ref, 4 * HD), proj(wk_ref, 2 * HD), proj(wv_ref, 2 * HD)
        for i in range(2):
            heads = [q[:, 2 * i * HD:(2 * i + 1) * HD], q[:, (2 * i + 1) * HD:(2 * i + 2) * HD], k[:, i * HD:(i + 1) * HD]]
            for part, (val, gain) in enumerate(zip(heads, (gq, gq, gk))):
                raw_ref[:, :, :, pl.ds(pl.multiple_of((2 * j + i) * 3 * HD + part * HD, HD), HD)] = val.reshape(shape)
                rot_ref[:, :, :, pl.ds(pl.multiple_of((2 * j + i) * 4 * HD + part * HD, HD), HD)] = post(val, gain)
            rot_ref[:, :, :, pl.ds(pl.multiple_of((2 * j + i) * 4 * HD + 3 * HD, HD), HD)] = v[:, i * HD:(i + 1) * HD].reshape(shape)
        return 0

    lax.fori_loop(0, wk_ref.shape[1] // (2 * HD), body, 0, unroll=2)


QB = 256
NT = (((1,), (1,)), ((), ()))
EXP_SCALE = HD ** -0.5 * math.log2(math.e)


def softmax_t(k, q, qb):
    lo = qb * QB
    parts = [(lo, lax.dot_general(k[lo:lo + QB], q, NT, preferred_element_type=F32))]
    keys = lax.broadcasted_iota(jnp.int32, (QB, QB), 0)
    queries = lax.broadcasted_iota(jnp.int32, (QB, QB), 1)
    parts[0] = (lo, jnp.where(keys <= queries, parts[0][1], -1e30))
    if lo:
        parts.append((0, lax.dot_general(k[:lo], q, NT, preferred_element_type=F32)))
    top = functools.reduce(jnp.maximum, [jnp.max(s, axis=0, keepdims=True) for _, s in parts])
    exps = [(at, jnp.exp2((s - top) * EXP_SCALE)) for at, s in parts]
    inv = 1.0 / functools.reduce(jnp.add, [jnp.sum(e, axis=0, keepdims=True) for _, e in exps])
    return [(at, e * inv) for at, e in exps]


def attn_fwd_kernel(rot_ref, o_ref):
    n_pos = rot_ref.shape[0] * rot_ref.shape[2]
    rot = rot_ref[...].reshape(n_pos, 4 * HD)
    k, v_t = rot[:, 2 * HD:3 * HD], rot[:, 3 * HD:].T
    src_b = QB // rot_ref.shape[2]
    for qb in range(n_pos // QB):
        for head in range(2):
            q = rot[qb * QB:(qb + 1) * QB, head * HD:(head + 1) * HD]
            o_t = functools.reduce(jnp.add, [
                jnp.dot(v_t[:, at:at + p.shape[0]], p.astype(BF16), preferred_element_type=F32)
                for at, p in softmax_t(k, q, qb)])
            o_ref[pl.ds(qb * src_b, src_b), 0, :, pl.ds(head * HD, HD)] = o_t.T.astype(BF16).reshape(src_b, o_ref.shape[2], HD)


MESH = pl.DeviceIdType.MESH


class Reducer:
    def __init__(self, chunks, acc, r1, r2, r3, send, recv, loc):
        self.chunks, self.acc, self.r1, self.r2, self.r3 = chunks, acc, r1, r2, r3
        self.send, self.recv, self.loc = send, recv, loc
        me = lax.axis_index('sp')
        self.me, self.c, self.x, self.y = me, me % 2, (me // 2) % 2, me // 4
        self.pn, self.xn, self.yn = me + 1 - 2 * self.c, me + 2 - 4 * self.x, me + 4 - 8 * self.y

    def barrier(self, n_dev):
        sem = pltpu.get_barrier_semaphore()
        for d in range(1, n_dev):
            pl.semaphore_signal(sem, inc=1, device_id=((self.me + d) % n_dev,), device_id_type=MESH)
        pl.semaphore_wait(sem, n_dev - 1)

    def rdma(self, src, dst, ci, slot, dev):
        return pltpu.make_async_remote_copy(src_ref=src, dst_ref=dst, send_sem=self.send.at[ci, slot], recv_sem=self.recv.at[ci, slot],
                                            device_id=(dev,), device_id_type=MESH)

    @staticmethod
    def rows(ref, at, n):
        return ref.at[pl.ds(pl.multiple_of(at, 8), n), :]

    def remote(self, i, k):
        src, out, row0, n = self.chunks[i]
        c, x, y, pn, xn, yn = self.c, self.x, self.y, self.pn, self.xn, self.yn
        acc, rows = self.acc[i], self.rows
        half, e, f = n // 2, n // 8, n // 16
        base = row0 + c * half
        p1, q1 = x * e, n // 4 + y * e
        p, q = p1 + y * f, q1 + x * f
        if k == 1:
            return [self.rdma(rows(src, row0 + (1 - c) * half, half), self.r1[i], i, 0, pn)]
        if k == 2:
            return [self.rdma(rows(acc, (1 - x) * e, e), self.r2[i].at[0], i, 1, xn),
                    self.rdma(rows(acc, n // 4 + (1 - y) * e, e), self.r2[i].at[1], i, 2, yn)]
        if k == 3:
            return [self.rdma(rows(acc, p1 + (1 - y) * f, f), self.r3[i].at[0], i, 3, yn),
                    self.rdma(rows(acc, q1 + (1 - x) * f, f), self.r3[i].at[1], i, 4, xn)]
        if k == 4:
            ps, qs, po, qo = rows(acc, p, f), rows(acc, q, f), rows(out, base + p, f), rows(out, base + q, f)
            return [self.rdma(ps, po, i, 5, yn), self.rdma(qs, qo, i, 6, xn), self.rdma(ps, po, i, 7, xn), self.rdma(qs, qo, i, 8, yn)]
        if k == 5:
            po, qo = rows(out, base + p1 + (1 - y) * f, f), rows(out, base + q1 + (1 - x) * f, f)
            return [self.rdma(po, po, i, 9, xn), self.rdma(qo, qo, i, 10, yn)]
        mine = rows(out, base, half)
        return [self.rdma(mine, mine, i, 11, pn)]

    def local(self, i, k):
        src, out, row0, n = self.chunks[i]
        c, half, rows = self.c, n // 2, self.rows
        base = row0 + c * half
        if k == 1:
            return [pltpu.make_async_copy(rows(src, base, half), self.acc[i], self.loc.at[i, 0])]
        p, q = self.x * (n // 8) + self.y * (n // 16), n // 4 + self.y * (n // 8) + self.x * (n // 16)
        return [pltpu.make_async_copy(rows(self.acc[i], at, n // 16), rows(out, base + at, n // 16), self.loc.at[i, 1 + j]) for j, at in enumerate((p, q))]

    def add(self, i, at, src, n):
        dst = self.acc[i]

        def body(j, _):
            dst[pl.ds(pl.multiple_of(at + j * 8, 8), 8), :] += src[pl.ds(pl.multiple_of(j * 8, 8), 8), :]
            return 0

        lax.fori_loop(0, n // 8, body, 0, unroll=2)

    def stage(self, i, k):
        n = self.chunks[i][3]
        e, f = n // 8, n // 16
        p1, q1 = self.x * e, n // 4 + self.y * e
        if k == 2:
            self.local(i, 1)[0].wait()
        if k == 6:
            for cp in self.local(i, 4):
                cp.wait()
        before = self.remote(i, k - 1) if k > 1 else []
        if k == 5:
            before = before[:2]
        if k == 6:
            before = self.remote(i, 4)[2:] + before
        for cp in before:
            cp.wait_recv()
        if k == 2:
            self.add(i, 0, self.r1[i], n // 2)
        elif k == 3:
            self.add(i, p1, self.r2[i].at[0], e)
            self.add(i, q1, self.r2[i].at[1], e)
        elif k == 4:
            self.add(i, p1 + self.y * f, self.r3[i].at[0], f)
            self.add(i, q1 + self.x * f, self.r3[i].at[1], f)
        if k in (1, 4):
            for cp in self.local(i, k):
                cp.start()
        for cp in self.remote(i, k):
            cp.start()

    def drain(self):
        for i in range(len(self.chunks)):
            self.remote(i, 6)[0].wait_recv()
            for k in range(1, 7):
                for cp in self.remote(i, k):
                    cp.wait_send()


def reduce_scratch(sizes):
    dma, nc = pltpu.SemaphoreType.DMA, len(sizes)
    out = [pltpu.VMEM((r // 2, w), F32) for r, w in sizes] + [pltpu.VMEM((r // 2, w), F32) for r, w in sizes]
    out += [pltpu.VMEM((2, r // 8, w), F32) for r, w in sizes] + [pltpu.VMEM((2, r // 16, w), F32) for r, w in sizes]
    return out + [dma((nc, 12)), dma((nc, 12)), dma((nc, 3))]


def reducer(chunks, refs):
    nc = len(chunks)
    return Reducer(chunks, *(refs[i * nc:(i + 1) * nc] for i in range(4)), *refs[4 * nc:4 * nc + 3])


BWD_STAGES = {0: ((0, 1), (1, 1)), 3: ((0, 2), (1, 2)), 8: ((0, 3),), 12: ((1, 3),), 14: ((0, 4),), 16: ((1, 4),),
              20: ((0, 5),), 24: ((1, 5),), 27: ((0, 6),), 29: ((1, 6),)}


def attn_bwd_kernel(n_dev, rot_ref, raw_ref, do_ref, gq_ref, gk_ref, cos_ref, sin_ref, wo_part, oq_ref, ok_ref, ov_ref, dgq_ref, dgk_ref, wo_sum,
                    dk_acc, dv_acc, *refs):
    step = pl.program_id(0) * pl.num_programs(1) + pl.program_id(1)
    n_half = wo_part.shape[0] // 2
    red = reducer([(wo_part, wo_sum, 0, n_half), (wo_part, wo_sum, n_half, n_half)], refs)
    for at, todo in BWD_STAGES.items():
        @pl.when(step == at)
        def _():
            if at == 0:
                red.barrier(n_dev)
            for i, k in todo:
                red.stage(i, k)

    n_src, _, tok, _ = rot_ref.shape
    n_pos = n_src * tok
    rot = rot_ref[...].reshape(n_pos, 4 * HD)
    raw = raw_ref[...].reshape(n_pos, 3 * HD)
    d_o = do_ref[...].reshape(n_pos, 2 * HD)
    k, v = rot[:, 2 * HD:3 * HD], rot[:, 3 * HD:]
    k_t = k.astype(F32).T.astype(BF16)
    src_b = QB // tok
    first = jnp.logical_and(pl.program_id(0) == 0, pl.program_id(1) == 0)

    @pl.when(first)
    def _():
        dgq_ref[...] = jnp.zeros_like(dgq_ref)
        dgk_ref[...] = jnp.zeros_like(dgk_ref)

    def post_back(d, x_raw, gain, lo, dg_ref):
        cnt = d.shape[0]
        d = d.astype(BF16).astype(F32)
        c, s = cos_ref[pl.ds(lo, cnt), :], sin_ref[pl.ds(lo, cnt), :]
        dn = d * c + pltpu.roll(d * s, HD // 2, 1)
        x = x_raw.astype(F32)
        r = lax.rsqrt(jnp.mean(x * x, axis=-1, keepdims=True) + NORM_EPS)
        xh = x * r
        t = dn * xh
        dg_ref[...] += jnp.sum(t.reshape(cnt // 8, 8, HD), axis=0)
        dng = dn * gain
        return (r * (dng - xh * jnp.mean(dng * xh, axis=-1, keepdims=True))).astype(BF16)

    for qb in reversed(range(n_pos // QB)):
        last = qb == n_pos // QB - 1
        sl = slice(qb * QB, (qb + 1) * QB)
        for head in range(2):
            hs = slice(head * HD, (head + 1) * HD)
            q, dob = rot[sl, hs], d_o[sl, hs]
            ps = softmax_t(k, q, qb)
            dps = [lax.dot_general(v[at:at + p.shape[0]], dob, NT, preferred_element_type=F32) for at, p in ps]
            delta = functools.reduce(jnp.add, [jnp.sum(p * dp, axis=0, keepdims=True) for (_, p), dp in zip(ps, dps)])
            dq_t = None
            for (at, p), dp in zip(ps, dps):
                ds = (p * (dp - delta) * HD ** -0.5).astype(BF16)
                dq_p = jnp.dot(k_t[:, at:at + p.shape[0]], ds, preferred_element_type=F32)
                dq_t = dq_p if dq_t is None else dq_t + dq_p
                dv = jnp.dot(p.astype(BF16), dob, preferred_element_type=F32)
                dk = jnp.dot(ds, q, preferred_element_type=F32)
                rows = pl.ds(at, dk.shape[0])
                if last and head == 0:
                    dk_acc[rows, :] = dk
                    dv_acc[rows, :] = dv
                else:
                    dk_acc[rows, :] += dk
                    dv_acc[rows, :] += dv
            dq_raw = post_back(dq_t.T, raw[sl, hs], gq_ref[...], qb * QB, dgq_ref)
            oq_ref[pl.ds(qb * src_b, src_b), 0, :, pl.ds(head * HD, HD)] = dq_raw.reshape(src_b, tok, HD)
    dk_raw = post_back(dk_acc[...], raw[:, 2 * HD:], gk_ref[...], 0, dgk_ref)
    ok_ref[:, 0] = dk_raw.reshape(n_src, tok, HD)
    ov_ref[:, 0] = dv_acc[...].astype(BF16).reshape(n_src, tok, HD)

    @pl.when(step == pl.num_programs(0) * pl.num_programs(1) - 1)
    def _():
        red.drain()


def tail_kernel(n_dev, *refs):
    wq, wk, wv, dq, dk, dv, pq, pk, pv, x_hbm, dy_hbm, g_ref, dgq, dgk, oq, ok, ov, odx, ogains = refs[:19]
    chunks = [(wk, ok, 0, wk.shape[0]), (wv, ov, 0, wv.shape[0]), (wq, oq, 0, wq.shape[0] // 2), (wq, oq, wq.shape[0] // 2, wq.shape[0] // 2)]
    nc = len(chunks)
    red = reducer(chunks, refs[19:])
    (vq, vk, vv, bq, bk, bv, bx, by, dn, dxb, gpack, gbuf,
     xsend, xrecv, gsend, grecv, lsem, wsem, bsem) = refs[19 + 4 * nc + 3:]
    me, c, x, y = red.me, red.c, red.x, red.y
    red.barrier(n_dev)

    _, rows, tok, dim = x_hbm.shape
    sb = bx.shape[1]
    n_blk = n_dev // sb
    ntok = sb * rows * tok
    loads = [pltpu.make_async_copy(a, b, wsem.at[i]) for i, (a, b) in enumerate(((pq, vq), (pk, vk), (pv, vv)))]
    order = [(2 - 4 * x) // sb, (4 - 8 * y) // sb, (2 - 4 * x + 4 - 8 * y) // sb, 0]
    blocks = [me // sb + o for o in order]

    def fetch(b):
        src = pl.ds(pl.multiple_of(blocks[b] * sb, sb), sb)
        cps = [pltpu.make_async_copy(a.at[src], v.at[b % 2], bsem.at[b % 2, i])
               for i, (a, v) in enumerate(((dq, bq), (dk, bk), (dv, bv), (x_hbm, bx), (dy_hbm, by)))]
        for cp in cps:
            cp.start()
        return cps

    xcopies = []
    local_out = []

    def dx_block(b, fetched):
        for cp in fetched:
            cp.wait()

        def col(j, _):
            cols = pl.ds(pl.multiple_of(j * 256, 256), 256)
            dn[:, cols] = functools.reduce(jnp.add, [
                lax.dot_general(d[b % 2].reshape(ntok, d.shape[-1]), w[cols, :], NT, preferred_element_type=F32)
                for d, w in ((bq, vq), (bk, vk), (bv, vv))])
            return 0

        lax.fori_loop(0, dim // 256, col, 0)

        def tail_rows(j, _):
            part = pl.ds(pl.multiple_of(j * tok, tok), tok)
            si, ri = j // rows, j % rows
            d = dn[part, :]
            xv = bx[b % 2, si, ri].astype(F32)
            r = lax.rsqrt(jnp.mean(xv * xv, axis=-1, keepdims=True) + NORM_EPS)
            xh = xv * r
            gpack[:, pl.ds(0, dim)] += jnp.sum((d * xh).reshape(tok // 8, 8, dim), axis=0)
            dng = d * g_ref[...]
            dx = r * (dng - xh * jnp.mean(dng * xh, axis=-1, keepdims=True))
            dxb[b, si, ri] = (by[b % 2, si, ri].astype(F32) + dx).astype(BF16)
            return 0

        lax.fori_loop(0, sb * rows, tail_rows, 0)
        home = odx.at[pl.ds(pl.multiple_of(me * rows, rows), rows)]
        for si in range(sb):
            core = (c + si) % 2
            to = blocks[b] * sb + core
            if b == n_blk - 1 and si == 0:
                cp = pltpu.make_async_copy(dxb.at[b, core], home, lsem.at[0])
                local_out.append(cp)
            else:
                cp = pltpu.make_async_remote_copy(src_ref=dxb.at[b, core], dst_ref=home, send_sem=xsend.at[b, si], recv_sem=xrecv.at[b, si],
                                                  device_id=(to,), device_id_type=MESH)
                xcopies.append(cp)
            cp.start()

    for i in range(nc):
        red.stage(i, 1)
    for cp in loads:
        cp.start()
    fetched = {0: fetch(0)}
    gpack[:, pl.ds(0, dim)] = jnp.zeros((8, dim), F32)
    gpack[:, pl.ds(dim, HD)] = dgq[...]
    gpack[:, pl.ds(dim + HD, HD)] = dgk[...]
    fetched[1] = fetch(1)
    for i in range(nc):
        red.stage(i, 2)
    for cp in loads:
        cp.wait()
    dx_block(0, fetched[0])
    fetched[2] = fetch(2)
    red.stage(0, 3)
    red.stage(1, 3)
    dx_block(1, fetched[1])
    fetched[3] = fetch(3)
    red.stage(0, 4)
    red.stage(2, 3)
    red.stage(1, 4)
    red.stage(3, 3)
    dx_block(2, fetched[2])
    red.stage(0, 5)
    red.stage(2, 4)
    red.stage(1, 5)
    red.stage(3, 4)
    dx_block(3, fetched[3])
    gcopies = []
    for d in range(1, n_dev):
        cp = pltpu.make_async_remote_copy(src_ref=gpack, dst_ref=gbuf.at[d - 1], send_sem=gsend.at[d], recv_sem=grecv.at[d],
                                          device_id=((me + d) % n_dev,), device_id_type=MESH)
        cp.start()
        gcopies.append(cp)
    red.stage(0, 6)
    red.stage(2, 5)
    red.stage(1, 6)
    red.stage(3, 5)
    red.stage(2, 6)
    red.stage(3, 6)
    for cp in gcopies:
        cp.wait()
    total = gpack[...] + functools.reduce(jnp.add, [gbuf[d] for d in range(n_dev - 1)])
    ogains[...] = jnp.sum(total, axis=0, keepdims=True)
    for cp in local_out:
        cp.wait()
    red.drain()
    for cp in xcopies:
        cp.wait()


def finish(n_dev, parts, d_parts, weights, x, dy, g2, dgq, dgk):
    dwq, dwk, dwv = parts
    nd, rows, tok, dim = x.shape
    sb = 2
    hbm, vmem = pl.BlockSpec(memory_space=pl.ANY), pl.BlockSpec(memory_space=pltpu.VMEM)
    sizes = [dwk.shape, dwv.shape] + [(dwq.shape[0] // 2, dwq.shape[1])] * 2
    dma = pltpu.SemaphoreType.DMA
    scratch = reduce_scratch(sizes)
    scratch += [pltpu.VMEM(w.shape, BF16) for w in weights]
    scratch += [pltpu.VMEM((2, sb, rows, tok, d.shape[-1]), BF16) for d in (*d_parts, x, dy)]
    scratch += [pltpu.VMEM((sb * rows * tok, dim), F32), pltpu.VMEM((nd // sb, sb, rows, tok, dim), BF16)]
    scratch += [pltpu.VMEM((8, dim + 2 * HD), F32), pltpu.VMEM((n_dev - 1, 8, dim + 2 * HD), F32)]
    scratch += [dma((nd // sb, sb)), dma((nd // sb, sb)), dma((n_dev,)), dma((n_dev,)), dma((1,)), dma((3,)), dma((2, 5))]
    return pl.pallas_call(
        functools.partial(tail_kernel, n_dev), in_specs=[hbm] * 11 + [vmem] * 3, out_specs=[hbm] * 4 + [vmem],
        out_shape=[jax.ShapeDtypeStruct(a.shape, F32) for a in parts] + [
            jax.ShapeDtypeStruct((nd * rows, tok, dim), BF16), jax.ShapeDtypeStruct((1, dim + 2 * HD), F32)],
        scratch_shapes=scratch, compiler_params=params(collective_id=0, has_side_effects=True), name='tail',
    )(*parts, *d_parts, *weights, x, dy, g2, dgq, dgk)


def params(**kw):
    return pltpu.CompilerParams(vmem_limit_bytes=VMEM_LIMIT, **kw)


def cost(flops, nbytes):
    return pl.CostEstimate(flops=int(flops), bytes_accessed=int(nbytes), transcendentals=0)


def solution(mesh):
    n_dev = mesh.shape['sp']
    seq_spec = P(None, 'sp', None)
    replicated = P()

    def local_step(hidden, norm_gain, w_q, w_k, w_v, q_gain, k_gain, w_o, d_out):
        n_batch, tok, dim = hidden.shape
        rows = n_batch // n_dev
        n_pos = tok * n_dev
        n_tok = n_pos * rows
        n_q, n_kv = w_q.shape[1] // HD, w_k.shape[1] // HD
        qw = n_q * HD
        cos_t, sin_t = rope_tables(n_pos)
        g2 = norm_gain.reshape(1, dim)
        gq2, gk2 = q_gain.reshape(1, HD), k_gain.reshape(1, HD)
        x = lax.all_to_all(hidden, 'sp', 0, 0, tiled=True).reshape(n_dev, rows, tok, dim)
        dy = lax.all_to_all(d_out, 'sp', 0, 0, tiled=True).reshape(n_dev, rows, tok, dim)

        sb = 2
        full = lambda *s: pl.BlockSpec(s, lambda *i: (0,) * len(s))
        tokspec = lambda c: pl.BlockSpec((sb, rows, tok, c), lambda i: (i, 0, 0, 0))
        shp = lambda c, d=BF16: jax.ShapeDtypeStruct((n_dev, rows, tok, c), d)
        h, raw, rot = pl.pallas_call(
            qkv_kernel, grid=(n_dev // sb,),
            in_specs=[tokspec(dim), full(1, dim), full(*w_q.shape), full(*w_k.shape), full(*w_v.shape), full(1, HD), full(1, HD),
                      pl.BlockSpec((sb * tok, HD), lambda i: (i, 0)), pl.BlockSpec((sb * tok, HD), lambda i: (i, 0))],
            out_specs=[tokspec(dim), tokspec(n_kv * 3 * HD), tokspec(n_kv * 4 * HD)],
            out_shape=[shp(dim), shp(n_kv * 3 * HD), shp(n_kv * 4 * HD)],
            compiler_params=params(), cost_estimate=cost(2 * n_tok * dim * 4 * HD * n_kv, 40e6), name='qkv',
        )(x, g2, w_q, w_k, w_v, gq2, gk2, cos_t, sin_t)

        head_spec = lambda c: pl.BlockSpec((n_dev, 1, tok, c), lambda r, j: (0, r, 0, j))
        o = pl.pallas_call(
            attn_fwd_kernel, grid=(rows, n_kv), in_specs=[head_spec(4 * HD)], out_specs=head_spec(2 * HD),
            out_shape=shp(qw), compiler_params=params(), cost_estimate=cost(4 * n_tok * n_pos * qw, 24e6), name='attn_fwd',
        )(rot)
        o2, dy2, x2 = o.reshape(n_tok, qw), dy.reshape(n_tok, dim), x.reshape(n_tok, dim)
        y = (x2.astype(F32) + jnp.dot(o2, w_o, preferred_element_type=F32)).astype(BF16)
        d_wo = lax.dot_general(o2, dy2, (((0,), (0,)), ((), ())), preferred_element_type=F32)
        d_o = lax.dot_general(dy2, w_o, (((1,), (1,)), ((), ())), preferred_element_type=F32).astype(BF16).reshape(n_dev, rows, tok, qw)
        y, d_wo, d_o = lax.optimization_barrier((y, d_wo, d_o))
        dq, dk, dv, dgq, dgk, d_wo = pl.pallas_call(
            functools.partial(attn_bwd_kernel, n_dev), grid=(rows, n_kv),
            in_specs=[head_spec(4 * HD), head_spec(3 * HD), head_spec(2 * HD), full(1, HD), full(1, HD), full(n_pos, HD), full(n_pos, HD),
                      pl.BlockSpec(memory_space=pl.ANY)],
            out_specs=[head_spec(2 * HD), head_spec(HD), head_spec(HD), full(8, HD), full(8, HD), pl.BlockSpec(memory_space=pl.ANY)],
            out_shape=[shp(qw), shp(n_kv * HD), shp(n_kv * HD), jax.ShapeDtypeStruct((8, HD), F32), jax.ShapeDtypeStruct((8, HD), F32),
                       jax.ShapeDtypeStruct(d_wo.shape, F32)],
            scratch_shapes=[pltpu.VMEM((n_pos, HD), F32), pltpu.VMEM((n_pos, HD), F32)] + reduce_scratch([(qw // 2, dim)] * 2),
            compiler_params=params(collective_id=1, has_side_effects=True), cost_estimate=cost(10 * n_tok * n_pos * qw, 60e6), name='attn_bwd',
        )(rot, raw, d_o, gq2, gk2, cos_t, sin_t, d_wo)
        y, dq = lax.optimization_barrier((y, dq))
        y_out = lax.all_to_all(y.reshape(n_batch, tok, dim), 'sp', 0, 0, tiled=True)
        h2 = h.reshape(n_tok, dim)
        d_wq, d_wk, d_wv = (lax.dot_general(h2, d.reshape(n_tok, -1), (((0,), (0,)), ((), ())), preferred_element_type=F32) for d in (dq, dk, dv))
        d_wq, d_wk, d_wv, d_hidden, gains = finish(n_dev, (d_wq, d_wk, d_wv), (dq, dk, dv), (w_q, w_k, w_v), x, dy, g2, dgq, dgk)
        gains = gains.reshape(-1)
        return (y_out, d_hidden, d_wq, d_wk, d_wv, d_wo, gains[:dim], gains[dim:dim + HD], gains[dim + HD:dim + 2 * HD])

    return jax.shard_map(local_step, mesh=mesh, in_specs=(seq_spec,) + (replicated,) * 7 + (seq_spec,),
                         out_specs=(seq_spec, seq_spec) + (replicated,) * 7, check_vma=False)
```

```python
import math
import functools
import jax
import jax.numpy as jnp
from jax import lax
from jax.experimental import pallas as pl
from jax.experimental.pallas import tpu as pltpu
from jax.sharding import PartitionSpec as P

ROPE_BASE = 1000000.0
NORM_EPS = 1e-6
F32 = jnp.float32
BF16 = jnp.bfloat16
HD = 128
VMEM_LIMIT = 60 * 1024 * 1024


def rope_tables(n_pos):
    half = HD // 2
    inv_freq = jnp.exp(jnp.arange(half).astype(F32) * (-2.0 * math.log(ROPE_BASE) / HD))
    angles = jnp.arange(n_pos).astype(F32)[:, None] * inv_freq[None, :]
    cos, sin = jnp.cos(angles), jnp.sin(angles)
    return jnp.concatenate([cos, cos], axis=-1), jnp.concatenate([-sin, sin], axis=-1)


def block_of(i):
    chip = lax.axis_index('sp') // 2
    return 2 * ((chip // 2 + i // 2) % 2) + (chip % 2 + i % 2) % 2


def qkv_kernel(n_dev, hid, dyl, g_ref, wq_ref, wk_ref, wv_ref, gq_ref, gk_ref, cos_ref, sin_ref, x_ref, h_ref, raw_ref, rot_ref, dy_hbm, xbuf, send, recv, dsend, drecv, lsem):
    n_src, rows, tok, dim = x_ref.shape
    n = n_src * rows * tok
    i = pl.program_id(0)
    me = lax.axis_index('sp')
    c = me % 2

    def piece(rel, si):
        core = (c + si) % 2
        to = block_of(rel) * 2 + core
        return pltpu.make_async_remote_copy(src_ref=hid.at[pl.ds(pl.multiple_of(to * rows, rows), rows)], dst_ref=xbuf.at[me],
                                            send_sem=send.at[rel, si], recv_sem=recv.at[rel, si], device_id=(to,), device_id_type=MESH)

    def dy_piece(si):
        to = block_of(3) * 2 + (c + si) % 2
        return pltpu.make_async_remote_copy(src_ref=dyl.at[pl.ds(pl.multiple_of(to * rows, rows), rows)], dst_ref=dy_hbm.at[me],
                                            send_sem=dsend.at[si], recv_sem=drecv.at[si], device_id=(to,), device_id_type=MESH)

    own = pltpu.make_async_copy(hid.at[pl.ds(pl.multiple_of(me * rows, rows), rows)], xbuf.at[me], lsem.at[0])
    n_rel = n_dev // 2

    @pl.when(i == 0)
    def _():
        own.start()
        sem = pltpu.get_barrier_semaphore()
        for d in range(1, n_dev):
            pl.semaphore_signal(sem, inc=1, device_id=((me + d) % n_dev,), device_id_type=MESH)
        pl.semaphore_wait(sem, n_dev - 1)
        for rel in range(n_rel):
            for si in range(2):
                if rel or si:
                    piece(rel, si).start()
        for si in range(2):
            dy_piece(si).start()
        own.wait()

    for rel in range(n_rel):
        @pl.when(i == rel)
        def _():
            for si in range(2):
                if rel or si:
                    piece(rel, si).wait_recv()

    @pl.when(i == n_rel - 1)
    def _():
        for rel in range(n_rel):
            for si in range(2):
                if rel or si:
                    piece(rel, si).wait_send()

    blk = block_of(i)
    x_ref[...] = xbuf[pl.ds(pl.multiple_of(blk * n_src, n_src), n_src)]
    x = x_ref[...].reshape(n, dim).astype(F32)
    r = lax.rsqrt(jnp.mean(x * x, axis=-1, keepdims=True) + NORM_EPS)
    h_ref[...] = (x * r * g_ref[...]).astype(BF16).reshape(h_ref.shape)
    at = pl.ds(pl.multiple_of(blk * n_src * tok, n_src * tok), n_src * tok)
    cos = cos_ref[at, :].reshape(n_src, 1, tok, HD)
    sin = sin_ref[at, :].reshape(n_src, 1, tok, HD)

    def post(raw, gain):
        v = raw.astype(F32)
        v = v * lax.rsqrt(jnp.mean(v * v, axis=-1, keepdims=True) + NORM_EPS) * gain
        rolled = pltpu.roll(v, HD // 2, 1).reshape(n_src, rows, tok, HD)
        return (v.reshape(n_src, rows, tok, HD) * cos + rolled * sin).astype(BF16)

    gq, gk = gq_ref[...], gk_ref[...]
    shape = (n_src, rows, tok, HD)

    def body(j, _):
        hh = h_ref[...].reshape(n, dim)

        def proj(w_ref, width):
            cols = pl.ds(pl.multiple_of(j * width, width), width)
            return jnp.dot(hh, w_ref[:, cols], preferred_element_type=F32).astype(BF16)

        q, k, v = proj(wq_ref, 4 * HD), proj(wk_ref, 2 * HD), proj(wv_ref, 2 * HD)
        for i in range(2):
            heads = [q[:, 2 * i * HD:(2 * i + 1) * HD], q[:, (2 * i + 1) * HD:(2 * i + 2) * HD], k[:, i * HD:(i + 1) * HD]]
            for part, (val, gain) in enumerate(zip(heads, (gq, gq, gk))):
                raw_ref[:, :, :, pl.ds(pl.multiple_of((2 * j + i) * 3 * HD + part * HD, HD), HD)] = val.reshape(shape)
                rot_ref[:, :, :, pl.ds(pl.multiple_of((2 * j + i) * 4 * HD + part * HD, HD), HD)] = post(val, gain)
            rot_ref[:, :, :, pl.ds(pl.multiple_of((2 * j + i) * 4 * HD + 3 * HD, HD), HD)] = v[:, i * HD:(i + 1) * HD].reshape(shape)
        return 0

    lax.fori_loop(0, wk_ref.shape[1] // (2 * HD), body, 0, unroll=2)

    @pl.when(i == n_rel - 1)
    def _():
        for si in range(2):
            dy_piece(si).wait()


QB_FWD, QB_BWD, KV_STEP = 512, 256, 2
NT = (((1,), (1,)), ((), ()))
EXP_SCALE = HD ** -0.5 * math.log2(math.e)


def softmax_t(k, q, qb):
    QB = q.shape[0]
    lo = qb * QB
    parts = [(lo, lax.dot_general(k[lo:lo + QB], q, NT, preferred_element_type=F32))]
    keys = lax.broadcasted_iota(jnp.int32, (QB, QB), 0)
    queries = lax.broadcasted_iota(jnp.int32, (QB, QB), 1)
    parts[0] = (lo, jnp.where(keys <= queries, parts[0][1], -1e30))
    if lo:
        parts.append((0, lax.dot_general(k[:lo], q, NT, preferred_element_type=F32)))
    top = functools.reduce(jnp.maximum, [jnp.max(s, axis=0, keepdims=True) for _, s in parts])
    exps = [(at, jnp.exp2((s - top) * EXP_SCALE)) for at, s in parts]
    inv = 1.0 / functools.reduce(jnp.add, [jnp.sum(e, axis=0, keepdims=True) for _, e in exps])
    return [(at, e * inv) for at, e in exps]


def attn_fwd_kernel(n_dev, rot_ref, x_ref, wo_ref, dyl, dy_part, o_ref, y_hbm, dy_hbm, o_all, yb, send, recv, lsem, dyb, dsend, drecv, dloc):
    n_src, _, tok, dim = x_ref.shape
    n_pos = n_src * tok
    r, j = pl.program_id(0), pl.program_id(1)
    n_rows, n_kv = dyl.shape[0] // n_dev, pl.num_programs(1)
    me = lax.axis_index('sp')

    c = me % 2

    def mine(dev):
        return dyl.at[pl.ds(pl.multiple_of(dev * n_rows, n_rows), n_rows)]

    def dy_piece(rel, si):
        to = block_of(rel) * 2 + (c + si) % 2
        return pltpu.make_async_remote_copy(src_ref=mine(to), dst_ref=dy_hbm.at[me], send_sem=dsend.at[rel, si], recv_sem=drecv.at[rel, si],
                                            device_id=(to,), device_id_type=MESH)

    dy_rest = ((0, 1), (1, 0), (2, 0), (1, 1), (2, 1))
    keep_in = pltpu.make_async_copy(mine(me), dyb, dloc.at[0])
    keep_out = pltpu.make_async_copy(dyb, dy_hbm.at[me], dloc.at[1])

    @pl.when(jnp.logical_and(r == 0, j == 0))
    def _():
        sem = pltpu.get_barrier_semaphore()
        for d in range(1, n_dev):
            pl.semaphore_signal(sem, inc=1, device_id=((me + d) % n_dev,), device_id_type=MESH)
        pl.semaphore_wait(sem, n_dev - 1)
        keep_in.start()
        for rel, si in dy_rest:
            dy_piece(rel, si).start()

    @pl.when(jnp.logical_and(r == 0, j == 1))
    def _():
        keep_in.wait()
        keep_out.start()

    rot = rot_ref[...].reshape(n_pos, 4 * HD)
    k, v_t = rot[:, 2 * HD:3 * HD], rot[:, 3 * HD:].T
    src_b = QB_FWD // tok
    for qb in range(n_pos // QB_FWD):
        for head in range(2):
            q = rot[qb * QB_FWD:(qb + 1) * QB_FWD, head * HD:(head + 1) * HD]
            o_t = functools.reduce(jnp.add, [
                jnp.dot(v_t[:, at:at + p.shape[0]], p.astype(BF16), preferred_element_type=F32)
                for at, p in softmax_t(k, q, qb)])
            o = o_t.T.astype(BF16)
            o_ref[pl.ds(qb * src_b, src_b), 0, :, pl.ds(head * HD, HD)] = o.reshape(src_b, tok, HD)
    o_all[j] = o_ref[...].reshape(n_pos, 2 * HD)

    def to_home(row, d):
        to = (me + d) % n_dev
        dst = y_hbm.at[me * n_rows + row]
        if d == 0:
            return pltpu.make_async_copy(yb.at[row, me], dst, lsem.at[row])
        return pltpu.make_async_remote_copy(src_ref=yb.at[row, to], dst_ref=dst, send_sem=send.at[row, d], recv_sem=recv.at[row, d],
                                            device_id=(to,), device_id_type=MESH)

    @pl.when(j == n_kv - 1)
    def _():
        width = 256

        def cols(t, _):
            at = pl.ds(pl.multiple_of(t * width, width), width)
            y = functools.reduce(jnp.add, [
                jnp.dot(o_all[kv], wo_ref[pl.ds(kv * 2 * HD, 2 * HD), at], preferred_element_type=F32) for kv in range(o_all.shape[0])])
            y = x_ref[:, 0, :, at].reshape(n_pos, width).astype(F32) + y
            yb[r, :, :, at] = y.astype(BF16).reshape(n_src, tok, width)
            return 0

        lax.fori_loop(0, dim // width, cols, 0)
        for d in range(n_dev):
            to_home(r, d).start()

    @pl.when(jnp.logical_and(r == n_rows - 1, j == n_kv - 1))
    def _():
        def finish_row(row, _):
            for d in range(n_dev):
                to_home(row, d).wait()
            return 0

        lax.fori_loop(0, n_rows, finish_row, 0)
        keep_out.wait()
        for rel, si in dy_rest:
            dy_piece(rel, si).wait()


MESH = pl.DeviceIdType.MESH


class Reducer:
    def __init__(self, chunks, acc, r1, r2, r3, send, recv, loc):
        self.chunks, self.acc, self.r1, self.r2, self.r3 = chunks, acc, r1, r2, r3
        self.send, self.recv, self.loc = send, recv, loc
        me = lax.axis_index('sp')
        self.me, self.c, self.x, self.y = me, me % 2, (me // 2) % 2, me // 4
        self.pn, self.xn, self.yn = me + 1 - 2 * self.c, me + 2 - 4 * self.x, me + 4 - 8 * self.y

    def barrier(self, n_dev):
        sem = pltpu.get_barrier_semaphore()
        for d in range(1, n_dev):
            pl.semaphore_signal(sem, inc=1, device_id=((self.me + d) % n_dev,), device_id_type=MESH)
        pl.semaphore_wait(sem, n_dev - 1)

    def rdma(self, src, dst, ci, slot, dev):
        return pltpu.make_async_remote_copy(src_ref=src, dst_ref=dst, send_sem=self.send.at[ci, slot], recv_sem=self.recv.at[ci, slot],
                                            device_id=(dev,), device_id_type=MESH)

    @staticmethod
    def rows(ref, at, n):
        return ref.at[pl.ds(pl.multiple_of(at, 8), n), :]

    def remote(self, i, k):
        src, out, row0, n = self.chunks[i]
        c, x, y, pn, xn, yn = self.c, self.x, self.y, self.pn, self.xn, self.yn
        acc, rows = self.acc[i], self.rows
        half, e, f = n // 2, n // 8, n // 16
        base = row0 + c * half
        p1, q1 = x * e, n // 4 + y * e
        p, q = p1 + y * f, q1 + x * f
        if k == 1:
            return [self.rdma(rows(src, row0 + (1 - c) * half, half), self.r1[i], i, 0, pn)]
        if k == 2:
            return [self.rdma(rows(acc, (1 - x) * e, e), self.r2[i].at[0], i, 1, xn),
                    self.rdma(rows(acc, n // 4 + (1 - y) * e, e), self.r2[i].at[1], i, 2, yn)]
        if k == 3:
            return [self.rdma(rows(acc, p1 + (1 - y) * f, f), self.r3[i].at[0], i, 3, yn),
                    self.rdma(rows(acc, q1 + (1 - x) * f, f), self.r3[i].at[1], i, 4, xn)]
        if k == 4:
            ps, qs, po, qo = rows(acc, p, f), rows(acc, q, f), rows(out, base + p, f), rows(out, base + q, f)
            return [self.rdma(ps, po, i, 5, yn), self.rdma(qs, qo, i, 6, xn), self.rdma(ps, po, i, 7, xn), self.rdma(qs, qo, i, 8, yn)]
        if k == 5:
            po, qo = rows(out, base + p1 + (1 - y) * f, f), rows(out, base + q1 + (1 - x) * f, f)
            return [self.rdma(po, po, i, 9, xn), self.rdma(qo, qo, i, 10, yn)]
        mine = rows(out, base, half)
        return [self.rdma(mine, mine, i, 11, pn)]

    def local(self, i, k):
        src, out, row0, n = self.chunks[i]
        c, half, rows = self.c, n // 2, self.rows
        base = row0 + c * half
        if k == 1:
            return [pltpu.make_async_copy(rows(src, base, half), self.acc[i], self.loc.at[i, 0])]
        p, q = self.x * (n // 8) + self.y * (n // 16), n // 4 + self.y * (n // 8) + self.x * (n // 16)
        return [pltpu.make_async_copy(rows(self.acc[i], at, n // 16), rows(out, base + at, n // 16), self.loc.at[i, 1 + j]) for j, at in enumerate((p, q))]

    def add(self, i, at, src, n):
        dst = self.acc[i]

        def body(j, _):
            dst[pl.ds(pl.multiple_of(at + j * 8, 8), 8), :] += src[pl.ds(pl.multiple_of(j * 8, 8), 8), :]
            return 0

        lax.fori_loop(0, n // 8, body, 0, unroll=2)

    def stage(self, i, k):
        n = self.chunks[i][3]
        e, f = n // 8, n // 16
        p1, q1 = self.x * e, n // 4 + self.y * e
        if k == 2:
            self.local(i, 1)[0].wait()
        if k == 6:
            for cp in self.local(i, 4):
                cp.wait()
        before = self.remote(i, k - 1) if k > 1 else []
        if k == 5:
            before = before[:2]
        if k == 6:
            before = self.remote(i, 4)[2:] + before
        for cp in before:
            cp.wait_recv()
        if k == 2:
            self.add(i, 0, self.r1[i], n // 2)
        elif k == 3:
            self.add(i, p1, self.r2[i].at[0], e)
            self.add(i, q1, self.r2[i].at[1], e)
        elif k == 4:
            self.add(i, p1 + self.y * f, self.r3[i].at[0], f)
            self.add(i, q1 + self.x * f, self.r3[i].at[1], f)
        if k in (1, 4):
            for cp in self.local(i, k):
                cp.start()
        for cp in self.remote(i, k):
            cp.start()

    def drain(self):
        for i in range(len(self.chunks)):
            self.remote(i, 6)[0].wait_recv()
            for k in range(1, 7):
                for cp in self.remote(i, k):
                    cp.wait_send()


def reduce_scratch(sizes):
    dma, nc = pltpu.SemaphoreType.DMA, len(sizes)
    out = [pltpu.VMEM((r // 2, w), F32) for r, w in sizes] + [pltpu.VMEM((r // 2, w), F32) for r, w in sizes]
    out += [pltpu.VMEM((2, r // 8, w), F32) for r, w in sizes] + [pltpu.VMEM((2, r // 16, w), F32) for r, w in sizes]
    return out + [dma((nc, 12)), dma((nc, 12)), dma((nc, 3))]


def reducer(chunks, refs):
    nc = len(chunks)
    return Reducer(chunks, *(refs[i * nc:(i + 1) * nc] for i in range(4)), *refs[4 * nc:4 * nc + 3])


BWD_STAGES = {0: ((0, 1), (1, 1)), 1: ((0, 2), (1, 2)), 4: ((0, 3),), 6: ((1, 3), (0, 4)), 8: ((1, 4),),
              10: ((0, 5),), 12: ((1, 5), (0, 6)), 14: ((1, 6),)}


def attn_bwd_kernel(n_dev, rot_ref, raw_ref, do_ref, gq_ref, gk_ref, cos_ref, sin_ref, wo_part, oq_ref, ok_ref, ov_ref, dgq_ref, dgk_ref, wo_sum,
                    dk_acc, dv_acc, *refs):
    step = pl.program_id(0) * pl.num_programs(1) + pl.program_id(1)
    n_half = wo_part.shape[0] // 2
    red = reducer([(wo_part, wo_sum, 0, n_half), (wo_part, wo_sum, n_half, n_half)], refs)
    for at, todo in BWD_STAGES.items():
        @pl.when(step == at)
        def _():
            if at == 0:
                red.barrier(n_dev)
            for i, k in todo:
                red.stage(i, k)

    n_src, _, tok, _ = rot_ref.shape
    n_pos = n_src * tok
    src_b = QB_BWD // tok
    first = jnp.logical_and(pl.program_id(0) == 0, pl.program_id(1) == 0)

    @pl.when(first)
    def _():
        dgq_ref[...] = jnp.zeros_like(dgq_ref)
        dgk_ref[...] = jnp.zeros_like(dgk_ref)

    def post_back(d, x_raw, gain, lo, dg_ref):
        cnt = d.shape[0]
        d = d.astype(BF16).astype(F32)
        c, s = cos_ref[pl.ds(lo, cnt), :], sin_ref[pl.ds(lo, cnt), :]
        dn = d * c + pltpu.roll(d * s, HD // 2, 1)
        x = x_raw.astype(F32)
        r = lax.rsqrt(jnp.mean(x * x, axis=-1, keepdims=True) + NORM_EPS)
        xh = x * r
        t = dn * xh
        dg_ref[...] += jnp.sum(t.reshape(cnt // 8, 8, HD), axis=0)
        dng = dn * gain
        return (r * (dng - xh * jnp.mean(dng * xh, axis=-1, keepdims=True))).astype(BF16)

    for kv in range(KV_STEP):
        rot = rot_ref[:, 0, :, pl.ds(kv * 4 * HD, 4 * HD)].reshape(n_pos, 4 * HD)
        raw = raw_ref[:, 0, :, pl.ds(kv * 3 * HD, 3 * HD)].reshape(n_pos, 3 * HD)
        d_o = do_ref[:, 0, :, pl.ds(kv * 2 * HD, 2 * HD)].reshape(n_pos, 2 * HD)
        k, v = rot[:, 2 * HD:3 * HD], rot[:, 3 * HD:]
        k_t = k.astype(F32).T.astype(BF16)
        for qb in reversed(range(n_pos // QB_BWD)):
            last = qb == n_pos // QB_BWD - 1
            sl = slice(qb * QB_BWD, (qb + 1) * QB_BWD)
            for head in range(2):
                hs = slice(head * HD, (head + 1) * HD)
                q, dob = rot[sl, hs], d_o[sl, hs]
                ps = softmax_t(k, q, qb)
                dps = [lax.dot_general(v[at:at + p.shape[0]], dob, NT, preferred_element_type=F32) for at, p in ps]
                delta = functools.reduce(jnp.add, [jnp.sum(p * dp, axis=0, keepdims=True) for (_, p), dp in zip(ps, dps)])
                dq_t = None
                for (at, p), dp in zip(ps, dps):
                    ds = (p * (dp - delta) * HD ** -0.5).astype(BF16)
                    dq_p = jnp.dot(k_t[:, at:at + p.shape[0]], ds, preferred_element_type=F32)
                    dq_t = dq_p if dq_t is None else dq_t + dq_p
                    dv = jnp.dot(p.astype(BF16), dob, preferred_element_type=F32)
                    dk = jnp.dot(ds, q, preferred_element_type=F32)
                    rows = pl.ds(at, dk.shape[0])
                    if last and head == 0:
                        dk_acc[kv, rows, :] = dk
                        dv_acc[kv, rows, :] = dv
                    else:
                        dk_acc[kv, rows, :] += dk
                        dv_acc[kv, rows, :] += dv
                dq_raw = post_back(dq_t.T, raw[sl, hs], gq_ref[...], qb * QB_BWD, dgq_ref)
                oq_ref[pl.ds(qb * src_b, src_b), 0, :, pl.ds((2 * kv + head) * HD, HD)] = dq_raw.reshape(src_b, tok, HD)
        dk_raw = post_back(dk_acc[kv], raw[:, 2 * HD:], gk_ref[...], 0, dgk_ref)
        ok_ref[:, 0, :, pl.ds(kv * HD, HD)] = dk_raw.reshape(n_src, tok, HD)
        ov_ref[:, 0, :, pl.ds(kv * HD, HD)] = dv_acc[kv].astype(BF16).reshape(n_src, tok, HD)

    @pl.when(step == pl.num_programs(0) * pl.num_programs(1) - 1)
    def _():
        red.drain()


def tail_kernel(n_dev, *refs):
    wq, wk, wv, dq, dk, dv, pq, pk, pv, x_hbm, dy_hbm, g_ref, dgq, dgk, oq, ok, ov, odx, ogains = refs[:19]
    chunks = [(wk, ok, 0, wk.shape[0]), (wv, ov, 0, wv.shape[0]), (wq, oq, 0, wq.shape[0] // 2), (wq, oq, wq.shape[0] // 2, wq.shape[0] // 2)]
    nc = len(chunks)
    red = reducer(chunks, refs[19:])
    (vq, vk, vv, bq, bk, bv, bx, by, dn, dxb, gpack, gbuf,
     xsend, xrecv, gsend, grecv, lsem, wsem, bsem) = refs[19 + 4 * nc + 3:]
    me, c, x, y = red.me, red.c, red.x, red.y
    red.barrier(n_dev)

    _, rows, tok, dim = x_hbm.shape
    sb = bx.shape[1]
    n_blk = n_dev // sb
    ntok = sb * rows * tok
    loads = [pltpu.make_async_copy(a, b, wsem.at[i]) for i, (a, b) in enumerate(((pq, vq), (pk, vk), (pv, vv)))]
    order = [(2 - 4 * x) // sb, (4 - 8 * y) // sb, (2 - 4 * x + 4 - 8 * y) // sb, 0]
    blocks = [me // sb + o for o in order]

    def fetch(b):
        src = pl.ds(pl.multiple_of(blocks[b] * sb, sb), sb)
        cps = [pltpu.make_async_copy(a.at[src], v.at[b % 2], bsem.at[b % 2, i])
               for i, (a, v) in enumerate(((dq, bq), (dk, bk), (dv, bv), (x_hbm, bx), (dy_hbm, by)))]
        for cp in cps:
            cp.start()
        return cps

    xcopies = []
    local_out = []

    def dx_block(b, fetched):
        for cp in fetched:
            cp.wait()

        def col(j, _):
            cols = pl.ds(pl.multiple_of(j * 256, 256), 256)
            dn[:, cols] = functools.reduce(jnp.add, [
                lax.dot_general(d[b % 2].reshape(ntok, d.shape[-1]), w[cols, :], NT, preferred_element_type=F32)
                for d, w in ((bq, vq), (bk, vk), (bv, vv))])
            return 0

        lax.fori_loop(0, dim // 256, col, 0)
        per = rows * tok

        def tail_rows(j, _):
            part = pl.ds(pl.multiple_of(j * tok, tok), tok)
            si, ri = j // rows, j % rows
            d = dn[part, :]
            xv = bx[b % 2, si, ri].astype(F32)
            r = lax.rsqrt(jnp.mean(xv * xv, axis=-1, keepdims=True) + NORM_EPS)
            xh = xv * r
            gpack[:, pl.ds(0, dim)] += jnp.sum((d * xh).reshape(tok // 8, 8, dim), axis=0)
            dng = d * g_ref[...]
            dx = r * (dng - xh * jnp.mean(dng * xh, axis=-1, keepdims=True))
            dxb[b, si, ri] = (by[b % 2, si, ri].astype(F32) + dx).astype(BF16)
            return 0

        lax.fori_loop(0, sb * rows, tail_rows, 0)

    def dx_send(b):
        home = odx.at[pl.ds(pl.multiple_of(me * rows, rows), rows)]
        for si in range(sb):
            core = (c + si) % 2
            to = blocks[b] * sb + core
            if b == n_blk - 1 and si == 0:
                cp = pltpu.make_async_copy(dxb.at[b, core], home, lsem.at[0])
                local_out.append(cp)
            else:
                cp = pltpu.make_async_remote_copy(src_ref=dxb.at[b, core], dst_ref=home, send_sem=xsend.at[b, si], recv_sem=xrecv.at[b, si],
                                                  device_id=(to,), device_id_type=MESH)
                xcopies.append(cp)
            cp.start()

    for i in range(nc):
        red.stage(i, 1)
    for cp in loads:
        cp.start()
    fetched = {0: fetch(0)}
    gpack[:, pl.ds(0, dim)] = jnp.zeros((8, dim), F32)
    gpack[:, pl.ds(dim, HD)] = dgq[...]
    gpack[:, pl.ds(dim + HD, HD)] = dgk[...]
    fetched[1] = fetch(1)
    for i in range(nc):
        red.stage(i, 2)
    for cp in loads:
        cp.wait()
    dx_block(0, fetched[0])
    dx_send(0)
    fetched[2] = fetch(2)
    red.stage(0, 3)
    dx_block(1, fetched[1])
    dx_send(1)
    fetched[3] = fetch(3)
    red.stage(1, 3)
    red.stage(0, 4)
    dx_block(2, fetched[2])
    red.stage(2, 3)
    red.stage(1, 4)
    dx_block(3, fetched[3])
    dx_send(3)
    gcopies = []
    for d in range(1, n_dev):
        cp = pltpu.make_async_remote_copy(src_ref=gpack, dst_ref=gbuf.at[d - 1], send_sem=gsend.at[d], recv_sem=grecv.at[d],
                                          device_id=((me + d) % n_dev,), device_id_type=MESH)
        cp.start()
        gcopies.append(cp)
    red.stage(3, 3)
    red.stage(2, 4)
    red.stage(0, 5)
    red.stage(1, 5)
    red.stage(3, 4)
    dx_send(2)
    red.stage(0, 6)
    red.stage(1, 6)
    red.stage(2, 5)
    red.stage(3, 5)
    red.stage(2, 6)
    red.stage(3, 6)
    for cp in gcopies:
        cp.wait()
    total = gpack[...] + functools.reduce(jnp.add, [gbuf[d] for d in range(n_dev - 1)])
    ogains[...] = jnp.sum(total, axis=0, keepdims=True)
    for cp in local_out:
        cp.wait()
    red.drain()
    for cp in xcopies:
        cp.wait()


def finish(n_dev, parts, d_parts, weights, x, dy, g2, dgq, dgk):
    dwq, dwk, dwv = parts
    nd, rows, tok, dim = x.shape
    sb = 2
    hbm, vmem = pl.BlockSpec(memory_space=pl.ANY), pl.BlockSpec(memory_space=pltpu.VMEM)
    sizes = [dwk.shape, dwv.shape] + [(dwq.shape[0] // 2, dwq.shape[1])] * 2
    dma = pltpu.SemaphoreType.DMA
    scratch = reduce_scratch(sizes)
    scratch += [pltpu.VMEM(w.shape, BF16) for w in weights]
    scratch += [pltpu.VMEM((2, sb, rows, tok, d.shape[-1]), BF16) for d in (*d_parts, x, dy)]
    scratch += [pltpu.VMEM((sb * rows * tok, dim), F32), pltpu.VMEM((nd // sb, sb, rows, tok, dim), BF16)]
    scratch += [pltpu.VMEM((8, dim + 2 * HD), F32), pltpu.VMEM((n_dev - 1, 8, dim + 2 * HD), F32)]
    scratch += [dma((nd // sb, sb)), dma((nd // sb, sb)), dma((n_dev,)), dma((n_dev,)), dma((1,)), dma((3,)), dma((2, 5))]
    return pl.pallas_call(
        functools.partial(tail_kernel, n_dev), in_specs=[hbm] * 11 + [vmem] * 3, out_specs=[hbm] * 4 + [vmem],
        out_shape=[jax.ShapeDtypeStruct(a.shape, F32) for a in parts] + [
            jax.ShapeDtypeStruct((nd * rows, tok, dim), BF16), jax.ShapeDtypeStruct((1, dim + 2 * HD), F32)],
        scratch_shapes=scratch, compiler_params=params(collective_id=0, has_side_effects=True), name='tail',
    )(*parts, *d_parts, *weights, x, dy, g2, dgq, dgk)


def params(**kw):
    return pltpu.CompilerParams(vmem_limit_bytes=VMEM_LIMIT, **kw)


def cost(flops, nbytes):
    return pl.CostEstimate(flops=int(flops), bytes_accessed=int(nbytes), transcendentals=0)


def solution(mesh):
    n_dev = mesh.shape['sp']
    seq_spec = P(None, 'sp', None)
    replicated = P()

    def local_step(hidden, norm_gain, w_q, w_k, w_v, q_gain, k_gain, w_o, d_out):
        n_batch, tok, dim = hidden.shape
        rows = n_batch // n_dev
        n_pos = tok * n_dev
        n_tok = n_pos * rows
        n_q, n_kv = w_q.shape[1] // HD, w_k.shape[1] // HD
        qw = n_q * HD
        cos_t, sin_t = rope_tables(n_pos)
        g2 = norm_gain.reshape(1, dim)
        gq2, gk2 = q_gain.reshape(1, HD), k_gain.reshape(1, HD)
        sb = 2
        full = lambda *s: pl.BlockSpec(s, lambda *i: (0,) * len(s))
        tokspec = lambda c: pl.BlockSpec((sb, rows, tok, c), lambda i: (i, 0, 0, 0))
        shp = lambda c, d=BF16: jax.ShapeDtypeStruct((n_dev, rows, tok, c), d)
        outspec = lambda c: pl.BlockSpec((sb, rows, tok, c), lambda i: (block_of(i), 0, 0, 0))
        hbm = pl.BlockSpec(memory_space=pl.ANY)
        dma = pltpu.SemaphoreType.DMA
        x, h, raw, rot, dy = pl.pallas_call(
            functools.partial(qkv_kernel, n_dev), grid=(n_dev // sb,),
            in_specs=[hbm, hbm, full(1, dim), full(*w_q.shape), full(*w_k.shape), full(*w_v.shape), full(1, HD), full(1, HD), full(n_pos, HD), full(n_pos, HD)],
            out_specs=[outspec(dim), outspec(dim), outspec(n_kv * 3 * HD), outspec(n_kv * 4 * HD), hbm],
            out_shape=[shp(dim), shp(dim), shp(n_kv * 3 * HD), shp(n_kv * 4 * HD), shp(dim)],
            scratch_shapes=[pltpu.VMEM((n_dev, rows, tok, dim), BF16), dma((n_dev // 2, 2)), dma((n_dev // 2, 2)), dma((2,)), dma((2,)), dma((1,))],
            compiler_params=params(collective_id=2, has_side_effects=True), cost_estimate=cost(2 * n_tok * dim * 4 * HD * n_kv, 40e6), name='qkv',
        )(hidden, d_out, g2, w_q, w_k, w_v, gq2, gk2, cos_t, sin_t)

        head_spec = lambda c: pl.BlockSpec((n_dev, 1, tok, c), lambda r, j: (0, r, 0, j))
        o, y_out, dy = pl.pallas_call(
            functools.partial(attn_fwd_kernel, n_dev), grid=(rows, n_kv),
            in_specs=[head_spec(4 * HD), pl.BlockSpec((n_dev, 1, tok, dim), lambda r, j: (0, r, 0, 0)), full(*w_o.shape), hbm, hbm],
            out_specs=[head_spec(2 * HD), hbm, hbm],
            out_shape=[shp(qw), jax.ShapeDtypeStruct((n_batch, tok, dim), BF16), shp(dim)], input_output_aliases={4: 2},
            scratch_shapes=[pltpu.VMEM((n_kv, n_pos, 2 * HD), BF16), pltpu.VMEM((rows, n_dev, tok, dim), BF16), dma((rows, n_dev)), dma((rows, n_dev)), dma((rows,)),
                            pltpu.VMEM((rows, tok, dim), BF16), dma((3, 2)), dma((3, 2)), dma((2,))],
            compiler_params=params(collective_id=3, has_side_effects=True), cost_estimate=cost(4 * n_tok * n_pos * qw, 24e6), name='attn_fwd',
        )(rot, x, w_o, d_out, dy)
        o2, dy2 = o.reshape(n_tok, qw), dy.reshape(n_tok, dim)
        d_wo = lax.dot_general(o2, dy2, (((0,), (0,)), ((), ())), preferred_element_type=F32)
        d_o = lax.dot_general(dy2, w_o, (((1,), (1,)), ((), ())), preferred_element_type=F32).astype(BF16).reshape(n_dev, rows, tok, qw)
        dq, dk, dv, dgq, dgk, d_wo = pl.pallas_call(
            functools.partial(attn_bwd_kernel, n_dev), grid=(rows, n_kv // KV_STEP),
            in_specs=[head_spec(KV_STEP * 4 * HD), head_spec(KV_STEP * 3 * HD), head_spec(KV_STEP * 2 * HD), full(1, HD), full(1, HD), full(n_pos, HD), full(n_pos, HD),
                      pl.BlockSpec(memory_space=pl.ANY)],
            out_specs=[head_spec(KV_STEP * 2 * HD), head_spec(KV_STEP * HD), head_spec(KV_STEP * HD), full(8, HD), full(8, HD), pl.BlockSpec(memory_space=pl.ANY)],
            out_shape=[shp(qw), shp(n_kv * HD), shp(n_kv * HD), jax.ShapeDtypeStruct((8, HD), F32), jax.ShapeDtypeStruct((8, HD), F32),
                       jax.ShapeDtypeStruct(d_wo.shape, F32)],
            scratch_shapes=[pltpu.VMEM((KV_STEP, n_pos, HD), F32), pltpu.VMEM((KV_STEP, n_pos, HD), F32)] + reduce_scratch([(qw // 2, dim)] * 2),
            compiler_params=params(collective_id=1, has_side_effects=True), cost_estimate=cost(10 * n_tok * n_pos * qw, 60e6), name='attn_bwd',
        )(rot, raw, d_o, gq2, gk2, cos_t, sin_t, d_wo)
        h2 = h.reshape(n_tok, dim)
        d_wq, d_wk, d_wv = (lax.dot_general(h2, d.reshape(n_tok, -1), (((0,), (0,)), ((), ())), preferred_element_type=F32) for d in (dq, dk, dv))
        d_wq, d_wk, d_wv, d_hidden, gains = finish(n_dev, (d_wq, d_wk, d_wv), (dq, dk, dv), (w_q, w_k, w_v), x, dy, g2, dgq, dgk)
        gains = gains.reshape(-1)
        return (y_out, d_hidden, d_wq, d_wk, d_wv, d_wo, gains[:dim], gains[dim:dim + HD], gains[dim + HD:dim + 2 * HD])

    return jax.shard_map(local_step, mesh=mesh, in_specs=(seq_spec,) + (replicated,) * 7 + (seq_spec,),
                         out_specs=(seq_spec, seq_spec) + (replicated,) * 7, check_vma=False)
```

```python
import math
import functools
import jax
import jax.numpy as jnp
from jax import lax
from jax.experimental import pallas as pl
from jax.experimental.pallas import tpu as pltpu
from jax.sharding import PartitionSpec as P

ROPE_BASE = 1000000.0
NORM_EPS = 1e-6
F32 = jnp.float32
BF16 = jnp.bfloat16
HD = 128
H2, H3, H4 = 2 * HD, 3 * HD, 4 * HD
VMEM_LIMIT = 60 * 1024 * 1024


def rope_tables(n_pos):
    half = HD // 2
    inv_freq = jnp.exp(jnp.arange(half).astype(F32) * (-2.0 * math.log(ROPE_BASE) / HD))
    angles = jnp.arange(n_pos).astype(F32)[:, None] * inv_freq[None, :]
    cos, sin = jnp.cos(angles), jnp.sin(angles)
    return jnp.concatenate([cos, cos], axis=-1), jnp.concatenate([-sin, sin], axis=-1)


def block_of(i):
    chip = lax.axis_index('sp') // 2
    return 2 * ((chip // 2 + i // 2) % 2) + (chip % 2 + i % 2) % 2


def qkv_kernel(n_dev, hid, dyl, g_ref, wq_ref, wk_ref, wv_ref, gq_ref, gk_ref, cos_ref, sin_ref, x_ref, h_ref, raw_ref, rot_ref, dy_hbm, xbuf, send, recv, dsend, drecv, lsem):
    n_src, rows, tok, dim = x_ref.shape
    n = n_src * rows * tok
    i = pl.program_id(0)
    me = lax.axis_index('sp')
    c = me % 2

    def piece(rel, si):
        core = (c + si) % 2
        to = block_of(rel) * 2 + core
        return pltpu.make_async_remote_copy(src_ref=hid.at[pl.ds(pl.multiple_of(to * rows, rows), rows)], dst_ref=xbuf.at[me],
                                            send_sem=send.at[rel, si], recv_sem=recv.at[rel, si], device_id=(to,), device_id_type=MESH)

    def dy_piece(si):
        to = block_of(3) * 2 + (c + si) % 2
        return pltpu.make_async_remote_copy(src_ref=dyl.at[pl.ds(pl.multiple_of(to * rows, rows), rows)], dst_ref=dy_hbm.at[me],
                                            send_sem=dsend.at[si], recv_sem=drecv.at[si], device_id=(to,), device_id_type=MESH)

    own = pltpu.make_async_copy(hid.at[pl.ds(pl.multiple_of(me * rows, rows), rows)], xbuf.at[me], lsem.at[0])
    n_rel = n_dev // 2

    @pl.when(i == 0)
    def _():
        own.start()
        sem = pltpu.get_barrier_semaphore()
        for d in range(1, n_dev):
            pl.semaphore_signal(sem, inc=1, device_id=((me + d) % n_dev,), device_id_type=MESH)
        pl.semaphore_wait(sem, n_dev - 1)
        for rel in range(n_rel):
            for si in range(2):
                if rel or si:
                    piece(rel, si).start()
        for si in range(2):
            dy_piece(si).start()
        own.wait()

    for rel in range(n_rel):
        @pl.when(i == rel)
        def _():
            for si in range(2):
                if rel or si:
                    piece(rel, si).wait_recv()

    @pl.when(i == n_rel - 1)
    def _():
        for rel in range(n_rel):
            for si in range(2):
                if rel or si:
                    piece(rel, si).wait_send()

    blk = block_of(i)
    x_ref[...] = xbuf[pl.ds(pl.multiple_of(blk * n_src, n_src), n_src)]
    x = x_ref[...].reshape(n, dim).astype(F32)
    r = lax.rsqrt(jnp.mean(x * x, axis=-1, keepdims=True) + NORM_EPS)
    h_ref[...] = (x * r * g_ref[...]).astype(BF16).reshape(h_ref.shape)
    at = pl.ds(pl.multiple_of(blk * n_src * tok, n_src * tok), n_src * tok)
    cos = cos_ref[at, :].reshape(n_src, 1, tok, HD)
    sin = sin_ref[at, :].reshape(n_src, 1, tok, HD)

    def post(raw, gain):
        v = raw.astype(F32)
        v = v * lax.rsqrt(jnp.mean(v * v, axis=-1, keepdims=True) + NORM_EPS) * gain
        rolled = pltpu.roll(v, HD // 2, 1).reshape(n_src, rows, tok, HD)
        return (v.reshape(n_src, rows, tok, HD) * cos + rolled * sin).astype(BF16)

    gq, gk = gq_ref[...], gk_ref[...]
    shape = (n_src, rows, tok, HD)

    def body(j, _):
        hh = h_ref[...].reshape(n, dim)

        def proj(w_ref, width):
            cols = pl.ds(pl.multiple_of(j * width, width), width)
            return jnp.dot(hh, w_ref[:, cols], preferred_element_type=F32).astype(BF16)

        q, k, v = proj(wq_ref, H4), proj(wk_ref, H2), proj(wv_ref, H2)
        for i in range(2):
            heads = [q[:, 2 * i * HD:(2 * i + 1) * HD], q[:, (2 * i + 1) * HD:(2 * i + 2) * HD], k[:, i * HD:(i + 1) * HD]]
            for part, (val, gain) in enumerate(zip(heads, (gq, gq, gk))):
                raw_ref[:, :, :, pl.ds(pl.multiple_of((2 * j + i) * H3 + part * HD, HD), HD)] = val.reshape(shape)
                rot_ref[:, :, :, pl.ds(pl.multiple_of((2 * j + i) * H4 + part * HD, HD), HD)] = post(val, gain)
            rot_ref[:, :, :, pl.ds(pl.multiple_of((2 * j + i) * H4 + H3, HD), HD)] = v[:, i * HD:(i + 1) * HD].reshape(shape)
        return 0

    lax.fori_loop(0, wk_ref.shape[1] // (H2), body, 0, unroll=2)

    @pl.when(i == n_rel - 1)
    def _():
        for si in range(2):
            dy_piece(si).wait()


QB_FWD, QB_BWD, KV_STEP = 512, 256, 2
NT = (((1,), (1,)), ((), ()))
TN = (((0,), (0,)), ((), ()))
EXP_SCALE = HD ** -0.5 * math.log2(math.e)


def softmax_t(k, q, qb):
    QB = q.shape[0]
    lo = qb * QB
    parts = [(lo, lax.dot_general(k[lo:lo + QB], q, NT, preferred_element_type=F32))]
    keys = lax.broadcasted_iota(jnp.int32, (QB, QB), 0)
    queries = lax.broadcasted_iota(jnp.int32, (QB, QB), 1)
    parts[0] = (lo, jnp.where(keys <= queries, parts[0][1], -1e30))
    if lo:
        parts.append((0, lax.dot_general(k[:lo], q, NT, preferred_element_type=F32)))
    top = functools.reduce(jnp.maximum, [jnp.max(s, axis=0, keepdims=True) for _, s in parts])
    exps = [(at, jnp.exp2((s - top) * EXP_SCALE)) for at, s in parts]
    inv = 1.0 / functools.reduce(jnp.add, [jnp.sum(e, axis=0, keepdims=True) for _, e in exps])
    return [(at, e * inv) for at, e in exps]


def attn_fwd_kernel(n_dev, rot_ref, x_ref, wo_ref, dyl, dy_part, o_ref, y_hbm, dy_hbm, o_all, yb, send, recv, lsem, dyb, dsend, drecv, dloc):
    n_src, _, tok, dim = x_ref.shape
    n_pos = n_src * tok
    r, j = pl.program_id(0), pl.program_id(1)
    n_rows, n_kv = dyl.shape[0] // n_dev, pl.num_programs(1)
    me = lax.axis_index('sp')

    c = me % 2

    def mine(dev):
        return dyl.at[pl.ds(pl.multiple_of(dev * n_rows, n_rows), n_rows)]

    def dy_piece(rel, si):
        to = block_of(rel) * 2 + (c + si) % 2
        return pltpu.make_async_remote_copy(src_ref=mine(to), dst_ref=dy_hbm.at[me], send_sem=dsend.at[rel, si], recv_sem=drecv.at[rel, si],
                                            device_id=(to,), device_id_type=MESH)

    dy_rest = ((0, 1), (1, 0), (2, 0), (1, 1), (2, 1))
    keep_in = pltpu.make_async_copy(mine(me), dyb, dloc.at[0])
    keep_out = pltpu.make_async_copy(dyb, dy_hbm.at[me], dloc.at[1])

    @pl.when(jnp.logical_and(r == 0, j == 0))
    def _():
        sem = pltpu.get_barrier_semaphore()
        for d in range(1, n_dev):
            pl.semaphore_signal(sem, inc=1, device_id=((me + d) % n_dev,), device_id_type=MESH)
        pl.semaphore_wait(sem, n_dev - 1)
        keep_in.start()
        for rel, si in dy_rest:
            dy_piece(rel, si).start()

    @pl.when(jnp.logical_and(r == 0, j == 1))
    def _():
        keep_in.wait()
        keep_out.start()

    rot = rot_ref[...].reshape(n_pos, H4)
    k, v_t = rot[:, H2:H3], rot[:, H3:].T
    src_b = QB_FWD // tok
    for qb in range(n_pos // QB_FWD):
        for head in range(2):
            q = rot[qb * QB_FWD:(qb + 1) * QB_FWD, head * HD:(head + 1) * HD]
            o_t = functools.reduce(jnp.add, [
                jnp.dot(v_t[:, at:at + p.shape[0]], p.astype(BF16), preferred_element_type=F32)
                for at, p in softmax_t(k, q, qb)])
            o = o_t.T.astype(BF16)
            o_ref[pl.ds(qb * src_b, src_b), 0, :, pl.ds(head * HD, HD)] = o.reshape(src_b, tok, HD)
    o_all[j] = o_ref[...].reshape(n_pos, H2)

    def to_home(row, d):
        to = (me + d) % n_dev
        dst = y_hbm.at[me * n_rows + row]
        if d == 0:
            return pltpu.make_async_copy(yb.at[row, me], dst, lsem.at[row])
        return pltpu.make_async_remote_copy(src_ref=yb.at[row, to], dst_ref=dst, send_sem=send.at[row, d], recv_sem=recv.at[row, d],
                                            device_id=(to,), device_id_type=MESH)

    @pl.when(j == n_kv - 1)
    def _():
        width = 256

        def cols(t, _):
            at = pl.ds(pl.multiple_of(t * width, width), width)
            y = functools.reduce(jnp.add, [
                jnp.dot(o_all[kv], wo_ref[pl.ds(kv * H2, H2), at], preferred_element_type=F32) for kv in range(o_all.shape[0])])
            y = x_ref[:, 0, :, at].reshape(n_pos, width).astype(F32) + y
            yb[r, :, :, at] = y.astype(BF16).reshape(n_src, tok, width)
            return 0

        lax.fori_loop(0, dim // width, cols, 0)
        for d in range(n_dev):
            to_home(r, d).start()

    @pl.when(jnp.logical_and(r == n_rows - 1, j == n_kv - 1))
    def _():
        def finish_row(row, _):
            for d in range(n_dev):
                to_home(row, d).wait()
            return 0

        lax.fori_loop(0, n_rows, finish_row, 0)
        keep_out.wait()
        for rel, si in dy_rest:
            dy_piece(rel, si).wait()


MESH = pl.DeviceIdType.MESH


class Reducer:
    def __init__(self, chunks, acc, r1, r2, r3, send, recv, loc):
        self.chunks, self.acc, self.r1, self.r2, self.r3 = chunks, acc, r1, r2, r3
        self.send, self.recv, self.loc = send, recv, loc
        me = lax.axis_index('sp')
        self.me, self.c, self.x, self.y = me, me % 2, (me // 2) % 2, me // 4
        self.pn, self.xn, self.yn = me + 1 - 2 * self.c, me + 2 - 4 * self.x, me + 4 - 8 * self.y

    def barrier(self, n_dev):
        sem = pltpu.get_barrier_semaphore()
        for d in range(1, n_dev):
            pl.semaphore_signal(sem, inc=1, device_id=((self.me + d) % n_dev,), device_id_type=MESH)
        pl.semaphore_wait(sem, n_dev - 1)

    def rdma(self, src, dst, ci, slot, dev):
        return pltpu.make_async_remote_copy(src_ref=src, dst_ref=dst, send_sem=self.send.at[ci, slot], recv_sem=self.recv.at[ci, slot],
                                            device_id=(dev,), device_id_type=MESH)

    @staticmethod
    def rows(ref, at, n):
        return ref.at[pl.ds(pl.multiple_of(at, 8), n), :]

    def remote(self, i, k):
        src, out, row0, n = self.chunks[i]
        c, x, y, pn, xn, yn = self.c, self.x, self.y, self.pn, self.xn, self.yn
        acc, rows = self.acc[i], self.rows
        half, e, f = n // 2, n // 8, n // 16
        base = row0 + c * half
        p1, q1 = x * e, n // 4 + y * e
        p, q = p1 + y * f, q1 + x * f
        if k == 1:
            return [self.rdma(rows(src, row0 + (1 - c) * half, half), self.r1[i], i, 0, pn)]
        if k == 2:
            return [self.rdma(rows(acc, (1 - x) * e, e), self.r2[i].at[0], i, 1, xn),
                    self.rdma(rows(acc, n // 4 + (1 - y) * e, e), self.r2[i].at[1], i, 2, yn)]
        if k == 3:
            return [self.rdma(rows(acc, p1 + (1 - y) * f, f), self.r3[i].at[0], i, 3, yn),
                    self.rdma(rows(acc, q1 + (1 - x) * f, f), self.r3[i].at[1], i, 4, xn)]
        if k == 4:
            ps, qs, po, qo = rows(acc, p, f), rows(acc, q, f), rows(out, base + p, f), rows(out, base + q, f)
            return [self.rdma(ps, po, i, 5, yn), self.rdma(qs, qo, i, 6, xn), self.rdma(ps, po, i, 7, xn), self.rdma(qs, qo, i, 8, yn)]
        if k == 5:
            po, qo = rows(out, base + p1 + (1 - y) * f, f), rows(out, base + q1 + (1 - x) * f, f)
            return [self.rdma(po, po, i, 9, xn), self.rdma(qo, qo, i, 10, yn)]
        mine = rows(out, base, half)
        return [self.rdma(mine, mine, i, 11, pn)]

    def local(self, i, k):
        src, out, row0, n = self.chunks[i]
        c, half, rows = self.c, n // 2, self.rows
        base = row0 + c * half
        if k == 1:
            return [pltpu.make_async_copy(rows(src, base, half), self.acc[i], self.loc.at[i, 0])]
        p, q = self.x * (n // 8) + self.y * (n // 16), n // 4 + self.y * (n // 8) + self.x * (n // 16)
        return [pltpu.make_async_copy(rows(self.acc[i], at, n // 16), rows(out, base + at, n // 16), self.loc.at[i, 1 + j]) for j, at in enumerate((p, q))]

    def add(self, i, at, src, n):
        dst = self.acc[i]

        def body(j, _):
            dst[pl.ds(pl.multiple_of(at + j * 8, 8), 8), :] += src[pl.ds(pl.multiple_of(j * 8, 8), 8), :]
            return 0

        lax.fori_loop(0, n // 8, body, 0, unroll=2)

    def stage(self, i, k):
        n = self.chunks[i][3]
        e, f = n // 8, n // 16
        p1, q1 = self.x * e, n // 4 + self.y * e
        if k == 2:
            self.local(i, 1)[0].wait()
        if k == 6:
            for cp in self.local(i, 4):
                cp.wait()
        before = self.remote(i, k - 1) if k > 1 else []
        if k == 5:
            before = before[:2]
        if k == 6:
            before = self.remote(i, 4)[2:] + before
        for cp in before:
            cp.wait_recv()
        if k == 2:
            self.add(i, 0, self.r1[i], n // 2)
        elif k == 3:
            self.add(i, p1, self.r2[i].at[0], e)
            self.add(i, q1, self.r2[i].at[1], e)
        elif k == 4:
            self.add(i, p1 + self.y * f, self.r3[i].at[0], f)
            self.add(i, q1 + self.x * f, self.r3[i].at[1], f)
        if k in (1, 4):
            for cp in self.local(i, k):
                cp.start()
        for cp in self.remote(i, k):
            cp.start()

    def drain(self):
        for i in range(len(self.chunks)):
            self.remote(i, 6)[0].wait_recv()
            for k in range(1, 7):
                for cp in self.remote(i, k):
                    cp.wait_send()


def reduce_scratch(sizes):
    dma, nc = pltpu.SemaphoreType.DMA, len(sizes)
    out = [pltpu.VMEM((r // 2, w), F32) for r, w in sizes] + [pltpu.VMEM((r // 2, w), F32) for r, w in sizes]
    out += [pltpu.VMEM((2, r // 8, w), F32) for r, w in sizes] + [pltpu.VMEM((2, r // 16, w), F32) for r, w in sizes]
    return out + [dma((nc, 12)), dma((nc, 12)), dma((nc, 3))]


def reducer(chunks, refs):
    nc = len(chunks)
    return Reducer(chunks, *(refs[i * nc:(i + 1) * nc] for i in range(4)), *refs[4 * nc:4 * nc + 3])


BWD_STAGES = ((0, 1, 4, 6, 10, 12), (0, 1, 6, 8, 12, 14))


def attn_bwd_kernel(n_dev, rot_ref, raw_ref, do_ref, gq_ref, gk_ref, cos_ref, sin_ref, wo_part, oq_ref, ok_ref, ov_ref, dgq_ref, dgk_ref, wo_sum,
                    dk_acc, dv_acc, *refs):
    step = pl.program_id(0) * pl.num_programs(1) + pl.program_id(1)
    n_half = wo_part.shape[0] // 2
    red = reducer([(wo_part, wo_sum, 0, n_half), (wo_part, wo_sum, n_half, n_half)], refs)
    for i, steps in enumerate(BWD_STAGES):
        for k, at in enumerate(steps):
            @pl.when(step == at)
            def _():
                if i + k == 0:
                    red.barrier(n_dev)
                red.stage(i, k + 1)

    n_src, _, tok, _ = rot_ref.shape
    n_pos = n_src * tok
    src_b = QB_BWD // tok
    first = jnp.logical_and(pl.program_id(0) == 0, pl.program_id(1) == 0)

    @pl.when(first)
    def _():
        dgq_ref[...] = jnp.zeros_like(dgq_ref)
        dgk_ref[...] = jnp.zeros_like(dgk_ref)

    def post_back(d, x_raw, gain, lo, dg_ref):
        cnt = d.shape[0]
        d = d.astype(BF16).astype(F32)
        c, s = cos_ref[pl.ds(lo, cnt), :], sin_ref[pl.ds(lo, cnt), :]
        dn = d * c + pltpu.roll(d * s, HD // 2, 1)
        x = x_raw.astype(F32)
        r = lax.rsqrt(jnp.mean(x * x, axis=-1, keepdims=True) + NORM_EPS)
        xh = x * r
        t = dn * xh
        dg_ref[...] += jnp.sum(t.reshape(cnt // 8, 8, HD), axis=0)
        dng = dn * gain
        return (r * (dng - xh * jnp.mean(dng * xh, axis=-1, keepdims=True))).astype(BF16)

    for kv in range(KV_STEP):
        rot = rot_ref[:, 0, :, pl.ds(kv * H4, H4)].reshape(n_pos, H4)
        raw = raw_ref[:, 0, :, pl.ds(kv * H3, H3)].reshape(n_pos, H3)
        d_o = do_ref[:, 0, :, pl.ds(kv * H2, H2)].reshape(n_pos, H2)
        k, v = rot[:, H2:H3], rot[:, H3:]
        k_t = k.astype(F32).T.astype(BF16)
        for qb in reversed(range(n_pos // QB_BWD)):
            last = qb == n_pos // QB_BWD - 1
            sl = slice(qb * QB_BWD, (qb + 1) * QB_BWD)
            for head in range(2):
                hs = slice(head * HD, (head + 1) * HD)
                q, dob = rot[sl, hs], d_o[sl, hs]
                ps = softmax_t(k, q, qb)
                dps = [lax.dot_general(v[at:at + p.shape[0]], dob, NT, preferred_element_type=F32) for at, p in ps]
                delta = functools.reduce(jnp.add, [jnp.sum(p * dp, axis=0, keepdims=True) for (_, p), dp in zip(ps, dps)])
                dq_t = None
                for (at, p), dp in zip(ps, dps):
                    ds = (p * (dp - delta) * HD ** -0.5).astype(BF16)
                    dq_p = jnp.dot(k_t[:, at:at + p.shape[0]], ds, preferred_element_type=F32)
                    dq_t = dq_p if dq_t is None else dq_t + dq_p
                    dv = jnp.dot(p.astype(BF16), dob, preferred_element_type=F32)
                    dk = jnp.dot(ds, q, preferred_element_type=F32)
                    rows = pl.ds(at, dk.shape[0])
                    if last and head == 0:
                        dk_acc[kv, rows, :] = dk
                        dv_acc[kv, rows, :] = dv
                    else:
                        dk_acc[kv, rows, :] += dk
                        dv_acc[kv, rows, :] += dv
                dq_raw = post_back(dq_t.T, raw[sl, hs], gq_ref[...], qb * QB_BWD, dgq_ref)
                oq_ref[pl.ds(qb * src_b, src_b), 0, :, pl.ds((2 * kv + head) * HD, HD)] = dq_raw.reshape(src_b, tok, HD)
        dk_raw = post_back(dk_acc[kv], raw[:, H2:], gk_ref[...], 0, dgk_ref)
        ok_ref[:, 0, :, pl.ds(kv * HD, HD)] = dk_raw.reshape(n_src, tok, HD)
        ov_ref[:, 0, :, pl.ds(kv * HD, HD)] = dv_acc[kv].astype(BF16).reshape(n_src, tok, HD)

    @pl.when(step == pl.num_programs(0) * pl.num_programs(1) - 1)
    def _():
        red.drain()


def tail_kernel(n_dev, *refs):
    wq, wk, wv, dq, dk, dv, pq, pk, pv, x_hbm, dy_hbm, g_ref, dgq, dgk, oq, ok, ov, odx, ogains = refs[:19]
    chunks = [(wk, ok, 0, wk.shape[0]), (wv, ov, 0, wv.shape[0]), (wq, oq, 0, wq.shape[0] // 2), (wq, oq, wq.shape[0] // 2, wq.shape[0] // 2)]
    nc = len(chunks)
    red = reducer(chunks, refs[19:])
    (vq, vk, vv, bq, bk, bv, bx, by, dn, dxb, gpack, gbuf,
     xsend, xrecv, gsend, grecv, lsem, wsem, bsem) = refs[19 + 4 * nc + 3:]
    me, c, x, y = red.me, red.c, red.x, red.y
    red.barrier(n_dev)

    _, rows, tok, dim = x_hbm.shape
    sb = bx.shape[1]
    n_blk = n_dev // sb
    ntok = sb * rows * tok
    loads = [pltpu.make_async_copy(a, b, wsem.at[i]) for i, (a, b) in enumerate(((pq, vq), (pk, vk), (pv, vv)))]
    order = [(2 - 4 * x) // sb, (4 - 8 * y) // sb, (2 - 4 * x + 4 - 8 * y) // sb, 0]
    blocks = [me // sb + o for o in order]

    def fetch(b):
        src = pl.ds(pl.multiple_of(blocks[b] * sb, sb), sb)
        cps = [pltpu.make_async_copy(a.at[src], v.at[b % 2], bsem.at[b % 2, i])
               for i, (a, v) in enumerate(((dq, bq), (dk, bk), (dv, bv), (x_hbm, bx), (dy_hbm, by)))]
        for cp in cps:
            cp.start()
        return cps

    xcopies = []
    local_out = []

    def dx_block(b, fetched):
        for cp in fetched:
            cp.wait()

        def col(j, _):
            cols = pl.ds(pl.multiple_of(j * 256, 256), 256)
            dn[:, cols] = functools.reduce(jnp.add, [
                lax.dot_general(d[b % 2].reshape(ntok, d.shape[-1]), w[cols, :], NT, preferred_element_type=F32)
                for d, w in ((bq, vq), (bk, vk), (bv, vv))])
            return 0

        lax.fori_loop(0, dim // 256, col, 0)
        per = rows * tok

        def tail_rows(j, _):
            part = pl.ds(pl.multiple_of(j * tok, tok), tok)
            si, ri = j // rows, j % rows
            d = dn[part, :]
            xv = bx[b % 2, si, ri].astype(F32)
            r = lax.rsqrt(jnp.mean(xv * xv, axis=-1, keepdims=True) + NORM_EPS)
            xh = xv * r
            gpack[:, pl.ds(0, dim)] += jnp.sum((d * xh).reshape(tok // 8, 8, dim), axis=0)
            dng = d * g_ref[...]
            dx = r * (dng - xh * jnp.mean(dng * xh, axis=-1, keepdims=True))
            dxb[b, si, ri] = (by[b % 2, si, ri].astype(F32) + dx).astype(BF16)
            return 0

        lax.fori_loop(0, sb * rows, tail_rows, 0)

    def dx_send(b):
        home = odx.at[pl.ds(pl.multiple_of(me * rows, rows), rows)]
        for si in range(sb):
            core = (c + si) % 2
            to = blocks[b] * sb + core
            if b == n_blk - 1 and si == 0:
                cp = pltpu.make_async_copy(dxb.at[b, core], home, lsem.at[0])
                local_out.append(cp)
            else:
                cp = pltpu.make_async_remote_copy(src_ref=dxb.at[b, core], dst_ref=home, send_sem=xsend.at[b, si], recv_sem=xrecv.at[b, si],
                                                  device_id=(to,), device_id_type=MESH)
                xcopies.append(cp)
            cp.start()

    for i in range(nc):
        red.stage(i, 1)
    for cp in loads:
        cp.start()
    fetched = {0: fetch(0)}
    gpack[:, pl.ds(0, dim)] = jnp.zeros((8, dim), F32)
    gpack[:, pl.ds(dim, HD)] = dgq[...]
    gpack[:, pl.ds(dim + HD, HD)] = dgk[...]
    fetched[1] = fetch(1)
    for i in range(nc):
        red.stage(i, 2)
    for cp in loads:
        cp.wait()
    late = n_blk - 2
    for b in range(n_blk):
        dx_block(b, fetched[b])
        if b != late:
            dx_send(b)
        if b + 2 < n_blk:
            fetched[b + 2] = fetch(b + 2)
        red.stage(b, 3)
        if b:
            red.stage(b - 1, 4)
    gcopies = []
    for d in range(1, n_dev):
        cp = pltpu.make_async_remote_copy(src_ref=gpack, dst_ref=gbuf.at[d - 1], send_sem=gsend.at[d], recv_sem=grecv.at[d],
                                          device_id=((me + d) % n_dev,), device_id_type=MESH)
        cp.start()
        gcopies.append(cp)
    first, last = range(nc // 2), range(nc // 2, nc)
    for i in first:
        red.stage(i, 5)
    red.stage(nc - 1, 4)
    dx_send(late)
    for i in first:
        red.stage(i, 6)
    for k in (5, 6):
        for i in last:
            red.stage(i, k)
    for cp in gcopies:
        cp.wait()
    total = gpack[...] + functools.reduce(jnp.add, [gbuf[d] for d in range(n_dev - 1)])
    ogains[...] = jnp.sum(total, axis=0, keepdims=True)
    for cp in local_out:
        cp.wait()
    red.drain()
    for cp in xcopies:
        cp.wait()


def finish(n_dev, parts, d_parts, weights, x, dy, g2, dgq, dgk):
    dwq, dwk, dwv = parts
    nd, rows, tok, dim = x.shape
    sb = 2
    hbm, vmem = pl.BlockSpec(memory_space=pl.ANY), pl.BlockSpec(memory_space=pltpu.VMEM)
    sizes = [dwk.shape, dwv.shape] + [(dwq.shape[0] // 2, dwq.shape[1])] * 2
    dma = pltpu.SemaphoreType.DMA
    scratch = reduce_scratch(sizes)
    scratch += [pltpu.VMEM(w.shape, BF16) for w in weights]
    scratch += [pltpu.VMEM((2, sb, rows, tok, d.shape[-1]), BF16) for d in (*d_parts, x, dy)]
    scratch += [pltpu.VMEM((sb * rows * tok, dim), F32), pltpu.VMEM((nd // sb, sb, rows, tok, dim), BF16)]
    scratch += [pltpu.VMEM((8, dim + H2), F32), pltpu.VMEM((n_dev - 1, 8, dim + H2), F32)]
    scratch += [dma((nd // sb, sb)), dma((nd // sb, sb)), dma((n_dev,)), dma((n_dev,)), dma((1,)), dma((3,)), dma((2, 5))]
    return pl.pallas_call(
        functools.partial(tail_kernel, n_dev), in_specs=[hbm] * 11 + [vmem] * 3, out_specs=[hbm] * 4 + [vmem],
        out_shape=[jax.ShapeDtypeStruct(a.shape, F32) for a in parts] + [
            jax.ShapeDtypeStruct((nd * rows, tok, dim), BF16), jax.ShapeDtypeStruct((1, dim + H2), F32)],
        scratch_shapes=scratch, compiler_params=params(collective_id=0, has_side_effects=True), name='tail',
    )(*parts, *d_parts, *weights, x, dy, g2, dgq, dgk)


def params(**kw):
    return pltpu.CompilerParams(vmem_limit_bytes=VMEM_LIMIT, **kw)


def solution(mesh):
    n_dev = mesh.shape['sp']
    seq_spec = P(None, 'sp', None)
    replicated = P()

    def local_step(hidden, norm_gain, w_q, w_k, w_v, q_gain, k_gain, w_o, d_out):
        n_batch, tok, dim = hidden.shape
        rows = n_batch // n_dev
        n_pos = tok * n_dev
        n_tok = n_pos * rows
        n_q, n_kv = w_q.shape[1] // HD, w_k.shape[1] // HD
        qw = n_q * HD
        cos_t, sin_t = rope_tables(n_pos)
        g2 = norm_gain.reshape(1, dim)
        gq2, gk2 = q_gain.reshape(1, HD), k_gain.reshape(1, HD)
        sb = 2
        full = lambda *s: pl.BlockSpec(s, lambda *i: (0,) * len(s))
        tokspec = lambda c: pl.BlockSpec((sb, rows, tok, c), lambda i: (i, 0, 0, 0))
        shp = lambda c, d=BF16: jax.ShapeDtypeStruct((n_dev, rows, tok, c), d)
        outspec = lambda c: pl.BlockSpec((sb, rows, tok, c), lambda i: (block_of(i), 0, 0, 0))
        hbm = pl.BlockSpec(memory_space=pl.ANY)
        dma = pltpu.SemaphoreType.DMA
        x, h, raw, rot, dy = pl.pallas_call(
            functools.partial(qkv_kernel, n_dev), grid=(n_dev // sb,),
            in_specs=[hbm, hbm, full(1, dim), full(*w_q.shape), full(*w_k.shape), full(*w_v.shape), full(1, HD), full(1, HD), full(n_pos, HD), full(n_pos, HD)],
            out_specs=[outspec(dim), outspec(dim), outspec(n_kv * H3), outspec(n_kv * H4), hbm],
            out_shape=[shp(dim), shp(dim), shp(n_kv * H3), shp(n_kv * H4), shp(dim)],
            scratch_shapes=[pltpu.VMEM((n_dev, rows, tok, dim), BF16), dma((n_dev // 2, 2)), dma((n_dev // 2, 2)), dma((2,)), dma((2,)), dma((1,))],
            compiler_params=params(collective_id=2, has_side_effects=True), name='qkv',
        )(hidden, d_out, g2, w_q, w_k, w_v, gq2, gk2, cos_t, sin_t)

        head_spec = lambda c: pl.BlockSpec((n_dev, 1, tok, c), lambda r, j: (0, r, 0, j))
        o, y_out, dy = pl.pallas_call(
            functools.partial(attn_fwd_kernel, n_dev), grid=(rows, n_kv),
            in_specs=[head_spec(H4), pl.BlockSpec((n_dev, 1, tok, dim), lambda r, j: (0, r, 0, 0)), full(*w_o.shape), hbm, hbm],
            out_specs=[head_spec(H2), hbm, hbm],
            out_shape=[shp(qw), jax.ShapeDtypeStruct((n_batch, tok, dim), BF16), shp(dim)], input_output_aliases={4: 2},
            scratch_shapes=[pltpu.VMEM((n_kv, n_pos, H2), BF16), pltpu.VMEM((rows, n_dev, tok, dim), BF16), dma((rows, n_dev)), dma((rows, n_dev)), dma((rows,)),
                            pltpu.VMEM((rows, tok, dim), BF16), dma((3, 2)), dma((3, 2)), dma((2,))],
            compiler_params=params(collective_id=3, has_side_effects=True), name='attn_fwd',
        )(rot, x, w_o, d_out, dy)
        o2, dy2 = o.reshape(n_tok, qw), dy.reshape(n_tok, dim)
        d_wo = lax.dot_general(o2, dy2, TN, preferred_element_type=F32)
        d_o = lax.dot_general(dy2, w_o, NT, preferred_element_type=F32).astype(BF16).reshape(n_dev, rows, tok, qw)
        dq, dk, dv, dgq, dgk, d_wo = pl.pallas_call(
            functools.partial(attn_bwd_kernel, n_dev), grid=(rows, n_kv // KV_STEP),
            in_specs=[head_spec(KV_STEP * H4), head_spec(KV_STEP * H3), head_spec(KV_STEP * H2), full(1, HD), full(1, HD), full(n_pos, HD), full(n_pos, HD),
                      pl.BlockSpec(memory_space=pl.ANY)],
            out_specs=[head_spec(KV_STEP * H2), head_spec(KV_STEP * HD), head_spec(KV_STEP * HD), full(8, HD), full(8, HD), pl.BlockSpec(memory_space=pl.ANY)],
            out_shape=[shp(qw), shp(n_kv * HD), shp(n_kv * HD), jax.ShapeDtypeStruct((8, HD), F32), jax.ShapeDtypeStruct((8, HD), F32),
                       jax.ShapeDtypeStruct(d_wo.shape, F32)],
            scratch_shapes=[pltpu.VMEM((KV_STEP, n_pos, HD), F32), pltpu.VMEM((KV_STEP, n_pos, HD), F32)] + reduce_scratch([(qw // 2, dim)] * 2),
            compiler_params=params(collective_id=1, has_side_effects=True), name='attn_bwd',
        )(rot, raw, d_o, gq2, gk2, cos_t, sin_t, d_wo)
        h2 = h.reshape(n_tok, dim)
        d_wq, d_wk, d_wv = (lax.dot_general(h2, d.reshape(n_tok, -1), TN, preferred_element_type=F32) for d in (dq, dk, dv))
        d_wq, d_wk, d_wv, d_hidden, gains = finish(n_dev, (d_wq, d_wk, d_wv), (dq, dk, dv), (w_q, w_k, w_v), x, dy, g2, dgq, dgk)
        gains = gains.reshape(-1)
        return (y_out, d_hidden, d_wq, d_wk, d_wv, d_wo, gains[:dim], gains[dim:dim + HD], gains[dim + HD:dim + H2])

    return jax.shard_map(local_step, mesh=mesh, in_specs=(seq_spec,) + (replicated,) * 7 + (seq_spec,),
                         out_specs=(seq_spec, seq_spec) + (replicated,) * 7, check_vma=False)
```
